512 devices in a mesh: mem: 64 (over z, x, core), gy: 8 (over y).
Axes of the slice: x: 4, y: 8, z: 8, core: 2. Of those that a mesh axis runs over, the one named last changes fastest.
Arguments:
- state: bfloat16 [64, 2, 2048, 1024], P('mem', None, None, 'gy'), may hold values from -6 to 6
- obs_index: int32 [64, 8, 256], P('mem', 'gy'), may hold values from 0 to 8191
- obs_count: int32 [64, 8], P('mem', 'gy'), may hold values from 1 to 256, as said below
- obs_value: float32 [64, 8, 256], P('mem', 'gy'), may hold values from -6 to 6
- obs_var: float32 [64, 8, 256], P('mem', 'gy'), may hold values from 0.1 to 1
- radius: int32 [64, 8], P('mem', 'gy'), may hold values from 8 to 16
Outputs:
- analysis: bfloat16 [64, 2, 2048, 1024], P('mem', None, None, 'gy')
The draws below stay inside these ranges and needn't reach their ends.
Inputs may be any that keep to these rules, and one draw needn't show every extreme that they name: `obs_count`: Tiles' counts are skewed: most tiles have few live slots, some many, and in every draw some tile has all 256 slots live.
All inputs are finite; a program needn't handle non-finite values.
Results may differ from the reference program's by a relative error of at most 0.0028.
The reference program's roundings to bfloat16 on the way (of `mixing`) count: a program that leaves them out, or rounds other values in their place, can miss the bound.
Values may be sent and summed in bfloat16 or wider, within the bound.
A program may use at most 64 MiB of HBM per device.

```python
import math
import jax
import jax.numpy as jnp
from jax import lax

K = 64
LEV = 2
ROWS = 128
COLS = 32
BLK = 16
OBS = 256
RMAX = 16
NSI = 10
TILES_X = 64
TILES_Y = 8
NXG = 2048
NYG = 1024
N_MEM = 64
N_GY = 8


def draw_obs_count(key, part):
    key_light = jax.random.fold_in(key, 11)
    key_heavy = jax.random.fold_in(key, 12)
    key_pick = jax.random.fold_in(key, 13)
    key_spot = jax.random.fold_in(key, 14)
    grid_shape = (TILES_X, TILES_Y)
    light = jax.random.randint(key_light, grid_shape, 1, OBS // 4 + 1)
    heavy = jax.random.randint(key_heavy, grid_shape, OBS // 2, OBS + 1)
    chosen = jax.random.randint(key_pick, grid_shape, 0, 4) == 0
    counts = jnp.where(chosen, heavy, light).reshape(-1)
    spot = jax.random.randint(key_spot, (), 0, TILES_X * TILES_Y)
    counts = jnp.where(jnp.arange(TILES_X * TILES_Y) == spot, OBS, counts)
    return counts.reshape(grid_shape).astype(jnp.int32)


def touch_ends(values, rng, least, top_value):
    extent = values.shape
    place = [jax.random.randint(jax.random.fold_in(rng, axis), (), 0, extent[axis]) for axis in range(len(extent))]
    values = values.at[tuple(place)].set(least)
    longest = extent.index(max(extent))
    place[longest] = (place[longest] + 1) % extent[longest]
    return values.at[tuple(place)].set(top_value)


def level_of(key, shape, pieces, smallest, largest):
    def one(axis_at, blocks):
        heights = jax.random.uniform(jax.random.fold_in(jax.random.fold_in(key, 6), axis_at), (blocks,), jnp.float32, smallest / len(pieces), largest / len(pieces))
        return jnp.repeat(jnp.exp(heights), shape[axis_at] // blocks).reshape((-1,) + (1,) * (len(shape) - axis_at - 1))

    level = one(*pieces[0])
    for cut in pieces[1:]:
        level = level * one(*cut)
    return level


def centred(key, extent, scale, bound, cuts=(), kind=jnp.bfloat16):
    level = level_of(key, extent, cuts, -0.22, 0.18) if cuts else 1.0
    entries = jax.random.normal(key, extent, jnp.float32) * scale * level
    return jnp.minimum(jnp.maximum(entries, -bound), bound).astype(kind)


def setup_inputs(seed: int = 0) -> dict:
    key_of = jax.random.split(jax.random.key(seed), 7)
    state = centred(key_of[0], (K, LEV, NXG, NYG), 1.0, 6.0, ((0, 64), (3, 8)))
    obs_index = touch_ends(jax.random.randint(key_of[1], (TILES_X, TILES_Y, OBS), 0, LEV * COLS * ROWS), jax.random.fold_in(key_of[1], 1), 0, (LEV * COLS * ROWS) - 1).astype(jnp.int32)
    obs_count = draw_obs_count(jax.random.fold_in(key_of[6], 71), 0)
    obs_value = centred(key_of[3], (TILES_X, TILES_Y, OBS), 1.0, 6.0, ((0, 64), (1, 8)), jnp.float32)
    obs_var = jnp.clip(jnp.exp(math.log(1.0) - 2.3025851 * jax.random.uniform(key_of[4], (TILES_X, TILES_Y, OBS), jnp.float32) ** level_of(key_of[4], (TILES_X, TILES_Y, OBS), ((0, 64), (1, 8)), -0.2, 0.2)), 0.1, 1.0)
    radius = touch_ends(jax.random.randint(key_of[5], (TILES_X, TILES_Y), RMAX // 2, RMAX + 1), jax.random.fold_in(key_of[5], 1), RMAX // 2, RMAX).astype(jnp.int32)
    return dict(state=state, obs_index=obs_index, obs_count=obs_count, obs_value=obs_value, obs_var=obs_var, radius=radius)


highest = lax.Precision.HIGHEST

def build_payload(ensemble, obs_slots, live_count, observed, variance):
    slot_total = obs_slots.shape[0]
    centre = lax.optimization_barrier(jnp.mean(ensemble, axis=0))
    spread = ensemble - centre
    is_live = jnp.arange(slot_total, dtype=jnp.int32) < live_count
    weight = jnp.where(is_live, 1.0 / variance, jnp.zeros_like(variance))
    innovation = observed - centre
    col_pos = (obs_slots // ROWS % COLS).astype(ensemble.dtype)
    row_pos = (obs_slots % ROWS).astype(ensemble.dtype)
    return jnp.concatenate([spread, innovation[None], weight[None], col_pos[None], row_pos[None]], axis=0)

def transforms(nearby, radius):
    dtype = nearby.dtype
    count_c = COLS // BLK
    count_r = ROWS // BLK
    block_ids = jnp.arange(count_c * count_r, dtype=jnp.int32)
    centre_c = (block_ids // count_r * BLK).astype(dtype) + (BLK - 1) / 2.0
    centre_r = (block_ids % count_r * BLK).astype(dtype) + (BLK - 1) / 2.0
    reach_sq = jnp.square(radius[0].astype(dtype))
    gram_sum = jnp.zeros((count_c * count_r, K, K), dtype)
    drive_sum = jnp.zeros((count_c * count_r, K), dtype)
    for step_x in range(3):
        for step_y in range(3):
            neighbour = nearby[step_x, step_y]
            spread = neighbour[:K]
            innovation = neighbour[K]
            weight = neighbour[K + 1]
            gap_c = (step_x - 1) * COLS + neighbour[K + 2][None, :] - centre_c[:, None]
            gap_r = (step_y - 1) * ROWS + neighbour[K + 3][None, :] - centre_r[:, None]
            taper_val = jnp.square(jnp.maximum(1.0 - (gap_c * gap_c + gap_r * gap_r) / reach_sq, 0.0))
            local_weight = taper_val * weight[None, :]
            weighted = local_weight[:, None, :] * spread[None]
            gram_sum = gram_sum + jnp.einsum('bko,jo->bkj', weighted, spread, precision=highest)
            drive_sum = drive_sum + jnp.einsum('bko,o->bk', weighted, innovation, precision=highest)
    identity = jnp.eye(K, dtype=dtype)
    system = (K - 1.0) * identity + gram_sum
    trace_scale = jnp.trace(system, axis1=1, axis2=2)
    upper_iter = system / trace_scale[:, None, None]
    lower_iter = jnp.broadcast_to(identity, system.shape)
    for sweep in range(NSI):
        factor = 1.5 * identity - 0.5 * jnp.einsum('bij,bjk->bik', lower_iter, upper_iter, precision=highest)
        upper_iter = jnp.einsum('bij,bjk->bik', upper_iter, factor, precision=highest)
        lower_iter = jnp.einsum('bij,bjk->bik', factor, lower_iter, precision=highest)
    inv_root = lower_iter / jnp.sqrt(trace_scale)[:, None, None]
    posterior = jnp.einsum('bij,bjk->bik', inv_root, inv_root, precision=highest)
    mean_shift = jnp.einsum('bkj,bj->bk', posterior, drive_sum, precision=highest)
    transform = jnp.sqrt(K - 1.0) * inv_root + mean_shift[:, :, None]
    mixing = 1.0 / K + transform - lax.optimization_barrier(jnp.mean(transform, axis=1, keepdims=True))
    return mixing.astype(jnp.bfloat16)

def mix_tile(tile_state, mixing):
    count_c = COLS // BLK
    count_r = ROWS // BLK
    blocks = tile_state.reshape(K, LEV, count_c, BLK, count_r, BLK).astype(jnp.float32)
    mix_table = mixing.reshape(count_c, count_r, K, K).astype(jnp.float32)
    mixed_tile = jnp.einsum('abkm,klaibj->mlaibj', mix_table, blocks)
    return mixed_tile.reshape(K, LEV, COLS, ROWS).astype(jnp.bfloat16)

def reference(state, obs_index, obs_count, obs_value, obs_var, radius):
    tiles_x = N_MEM
    tiles_y = N_GY
    anchor = jnp.zeros((), jnp.int32)

    def tile_at(tile_x, tile_y):
        return lax.dynamic_slice(state, (anchor, anchor, (tile_x * COLS).astype(jnp.int32), (tile_y * ROWS).astype(jnp.int32)), (K, LEV, COLS, ROWS))

    def payload_of(flat_id):
        tile_x = flat_id // tiles_y
        tile_y = flat_id % tiles_y
        tile_state = tile_at(tile_x, tile_y)
        obs_slots = obs_index[tile_x, tile_y]
        ensemble = jnp.take(tile_state.reshape(K, LEV * COLS * ROWS), obs_slots, axis=1).astype(jnp.float32)
        return build_payload(ensemble, obs_slots, obs_count[tile_x, tile_y], obs_value[tile_x, tile_y], obs_var[tile_x, tile_y])
    tile_ids = jnp.arange(tiles_x * tiles_y, dtype=jnp.int32)
    payloads = lax.map(payload_of, tile_ids).reshape(tiles_x, tiles_y, K + 4, OBS)
    padded = jnp.pad(payloads, ((1, 1), (1, 1), (0, 0), (0, 0)))

    def analyse(flat_id):
        tile_x = flat_id // tiles_y
        tile_y = flat_id % tiles_y
        nearby = lax.dynamic_slice(padded, (tile_x, tile_y, anchor, anchor), (3, 3, K + 4, OBS))
        return mix_tile(tile_at(tile_x, tile_y), transforms(nearby, radius[tile_x, tile_y][None]))
    result = lax.map(analyse, tile_ids)
    result = result.reshape(tiles_x, tiles_y, K, LEV, COLS, ROWS).transpose(2, 3, 0, 4, 1, 5)
    return result.reshape(K, LEV, tiles_x * COLS, tiles_y * ROWS)
```

```python
import functools

import jax
import jax.numpy as jnp
from jax import lax
from jax.experimental import pallas as pl
from jax.experimental.pallas import tpu as pltpu
from jax.sharding import PartitionSpec as P

K = 64
LEV = 2
ROWS = 128
COLS = 32
BLK = 16
OBS = 256
NSI = 10
N_MEM = 64
N_GY = 8
NR = ROWS // BLK
OWN = 4
GRAM_ROWS = NR * K + 16

MESH = pl.DeviceIdType.MESH
f32 = jnp.float32
bf16 = jnp.bfloat16

SIDES = [(dx, dy) for dx in (-1, 0, 1) for dy in (-1, 0, 1) if (dx, dy) != (0, 0)]


def split(x):
    hi = x.astype(bf16)
    lo = (x - hi.astype(f32)).astype(bf16)
    return hi, lo


def dot(a, b):
    return jnp.dot(a, b, preferred_element_type=f32)


def dot_nt(a, b):
    return lax.dot_general(a, b, (((1,), (1,)), ((), ())), preferred_element_type=f32)


def peer(me, step):
    j = step % 8
    r = step // 8
    dz = ((j + 1) // 2 * (2 * (j % 2) - 1) + 8) % 8
    dx = r // 2
    dc = r % 2
    z, x, c = me // 8, me // 2 % 4, me % 2
    target = (z + dz) % 8 * 8 + (x + dx) % 4 * 2 + (c + dc) % 2
    source = (z + 8 - dz) % 8 * 8 + (x + 4 - dx) % 4 * 2 + (c + 2 - dc) % 2
    return target, source


def kernel(
    state_ref, meta_ref, out_ref,
    tile_ref, mixed_ref, ens_ref, halo_ref, z_ref, o_ref, gram_ref,
    own_sem, in_send, in_recv, meta_send, meta_recv, ens_send, ens_recv, out_send, out_recv,
):
    me = lax.axis_index("mem")
    gy = lax.axis_index("gy")
    barrier = pltpu.get_barrier_semaphore()

    def greet(step, _):
        target, _source = peer(me, step)
        pl.semaphore_signal(barrier, inc=1, device_id=(target, gy), device_id_type=MESH)
        return 0

    lax.fori_loop(1, N_MEM, greet, 0)
    for dx, dy in SIDES:
        if dy != 0:
            device = ((me + dx + N_MEM) % N_MEM, (gy + dy + N_GY) % N_GY)
            pl.semaphore_signal(barrier, inc=1, device_id=device, device_id_type=MESH)
    pl.semaphore_wait(barrier, N_MEM - 1 + 6)

    def entry_copy(target, slot):
        return pltpu.make_async_remote_copy(
            src_ref=state_ref.at[0, :, pl.ds(pl.multiple_of(target * COLS, COLS), COLS), :],
            dst_ref=tile_ref.at[slot],
            send_sem=in_send.at[target],
            recv_sem=in_recv.at[slot],
            device_id=(target, gy),
            device_id_type=MESH,
        )

    def side_copy(src, dst, send, recv, index):
        dx, dy = SIDES[index]
        slot = (dx + 1) * 3 + dy + 1
        device = ((me - dx + N_MEM) % N_MEM, (gy - dy + N_GY) % N_GY)
        return pltpu.make_async_remote_copy(
            src_ref=src,
            dst_ref=dst.at[slot],
            send_sem=send.at[index],
            recv_sem=recv.at[index],
            device_id=device,
            device_id_type=MESH,
        )

    meta_copies = [side_copy(meta_ref, halo_ref, meta_send, meta_recv, i) for i in range(8)]
    for copy in meta_copies:
        copy.start()

    def start_entry(step, _):
        target, _source = peer(me, step)
        entry_copy(target, me).start()
        return 0

    lax.fori_loop(1, N_MEM, start_entry, 0)
    own_in = pltpu.make_async_copy(
        state_ref.at[0, :, pl.ds(pl.multiple_of(me * COLS, COLS), COLS), :],
        tile_ref.at[me],
        own_sem.at[0],
    )
    own_in.start()
    halo_ref[OWN] = meta_ref[...]
    own_in.wait()

    def finish_entry(step, _):
        target, source = peer(me, step)
        entry_copy(target, source).wait()
        return 0

    lax.fori_loop(1, N_MEM, finish_entry, 0)

    meta = meta_ref[...]
    pick_row = (
        lax.broadcasted_iota(jnp.int32, (ROWS, OBS), 0).astype(f32) == meta[3:4]
    ).astype(f32).astype(bf16)
    pick_col = lax.broadcasted_iota(jnp.int32, (LEV * COLS, OBS), 0).astype(f32) == meta[4:5]

    def observe(group, _):
        first = pl.multiple_of(group * 16, 16)
        cells = tile_ref[pl.ds(first, 16)].reshape(16 * LEV * COLS, ROWS)
        rows = dot(cells, pick_row).reshape(16, LEV * COLS, OBS)
        seen = jnp.sum(jnp.where(pick_col[None], rows, 0.0), axis=1)
        ens_ref[OWN, pl.ds(first, 16), :] = seen.astype(bf16)
        return 0

    lax.fori_loop(0, K // 16, observe, 0)

    ens_copies = [side_copy(ens_ref.at[OWN], ens_ref, ens_send, ens_recv, i) for i in range(8)]
    for copy in ens_copies:
        copy.start()
    for copy in meta_copies:
        copy.wait()
    for copy in ens_copies:
        copy.wait()

    left = lax.broadcasted_iota(jnp.int32, (K, 2 * K), 1) < K
    left_row = lax.broadcasted_iota(jnp.int32, (1, 2 * K), 1) < K
    lane = lax.broadcasted_iota(jnp.int32, (K, 2 * K), 1)
    eye = (lane % K == lax.broadcasted_iota(jnp.int32, (K, 2 * K), 0)).astype(f32)
    left_bf = jnp.where(left, 1.0, 0.0).astype(bf16)
    right_bf = jnp.where(left, 0.0, 1.0).astype(bf16)
    i_row = lax.broadcasted_iota(jnp.int32, (256, 256), 0)
    i_col = lax.broadcasted_iota(jnp.int32, (256, 256), 1)
    swap = jnp.where(
        (i_row // 16 == i_col % 16) & (i_row % 16 == i_col // 16), 1.0, 0.0
    ).astype(bf16)
    reach_sq = meta[5:6] * meta[5:6]
    centre_r = lax.broadcasted_iota(jnp.int32, (NR, OBS), 0).astype(f32) * BLK + (BLK - 1) / 2.0
    row_group = lax.broadcasted_iota(jnp.int32, (K, 2 * ROWS), 1) % ROWS // BLK
    group_masks = [jnp.where(row_group == r, 1.0, 0.0).astype(bf16) for r in range(NR)]

    def halves_sum(x):
        total = jnp.sum(x, axis=1, keepdims=True)
        first = jnp.sum(jnp.where(left, x, 0.0), axis=1, keepdims=True)
        return jnp.where(left, first, total - first)

    def halves_sum_exact(x):
        first = jnp.sum(jnp.where(left, x, 0.0), axis=1, keepdims=True)
        second = jnp.sum(jnp.where(left, 0.0, x), axis=1, keepdims=True)
        return jnp.where(left, first, second)

    def weighted(slot, dx, dy, a):
        ens = ens_ref[slot].astype(f32)
        about = halo_ref[slot]
        centre = jnp.sum(ens, axis=0, keepdims=True) * (1.0 / K)
        spread = ens - centre
        innovation = about[1:2] - centre
        inside = (me + dx >= 0) & (me + dx < N_MEM) & (gy + dy >= 0) & (gy + dy < N_GY)
        weight = about[0:1] * jnp.where(inside, 1.0, 0.0)
        centre_c = (a * BLK).astype(f32) + (BLK - 1) / 2.0
        gap_c = (dx * COLS) * 1.0 + about[2:3] - centre_c
        gap_r = (dy * ROWS) * 1.0 + about[3:4] - centre_r
        taper = jnp.square(jnp.maximum(1.0 - (gap_c * gap_c + gap_r * gap_r) / reach_sq, 0.0))
        rho = taper * weight
        drive = jnp.concatenate([rho * innovation, jnp.zeros((8, OBS), f32)], axis=0)
        hi, lo = split(spread)
        return rho, spread, drive, jnp.concatenate([hi, lo], axis=0)

    def product(parts, both):
        hi, lo = split(jnp.concatenate(parts, axis=0))
        return dot_nt(hi, both) + dot_nt(lo, both)

    def band(a, _):
        dx = 2 * a - 1
        side = 6 * a + 1
        rho, spread, drive, both = weighted(OWN, 0, 0, a)
        gram_ref[...] = product([rho[r : r + 1] * spread for r in range(NR)] + [drive], both)
        rho, spread, drive, both = weighted(side, dx, 0, a)
        gram_ref[...] += product([rho[r : r + 1] * spread for r in range(NR)] + [drive], both)
        for dy, r in ((-1, 0), (1, NR - 1)):
            for slot, step in ((OWN + dy, 0), (side + dy, dx)):
                rho, spread, drive, both = weighted(slot, step, dy, a)
                part = product([rho[r : r + 1] * spread, drive], both)
                gram_ref[r * K : (r + 1) * K, :] += part[:K]
                gram_ref[NR * K :, :] += part[K:]

        def folded(block):
            return block + pltpu.roll(block, K, 1)

        drives = folded(gram_ref[NR * K :, :])
        uppers, lowers, scales, drive_rows = [], [], [], []
        for pair in range(NR // 2):
            r = 2 * pair
            first = folded(gram_ref[r * K : (r + 1) * K, :])
            second = folded(gram_ref[(r + 1) * K : (r + 2) * K, :])
            system = (K - 1.0) * eye + jnp.where(left, first, second)
            diagonal = jnp.sum(system * eye, axis=0, keepdims=True)
            trace_l = jnp.sum(jnp.where(left_row, diagonal, 0.0), axis=1, keepdims=True)
            trace_r = jnp.sum(jnp.where(left_row, 0.0, diagonal), axis=1, keepdims=True)
            scale = jnp.where(left_row, trace_l, trace_r)
            scales.append(scale)
            drive_rows.append(jnp.where(left_row, drives[r : r + 1], drives[r + 1 : r + 2]))
            uppers.append(system / scale)

        def diag_rhs(hi, lo):
            def blocks(x):
                return jnp.concatenate([x * left_bf, x * right_bf], axis=0)

            return blocks(hi), blocks(lo)

        def times(hi, lo, rhs):
            rhs_hi, rhs_lo = rhs
            return dot(
                jnp.concatenate([hi, lo], axis=1), jnp.concatenate([rhs_hi, rhs_hi], axis=0)
            ) + dot(hi, rhs_lo)

        next_uppers = []
        for upper in uppers:
            hi, lo = split(upper)
            next_uppers.append(1.5 * upper - 0.5 * times(hi, lo, diag_rhs(hi, lo)))
            lowers.append(1.5 * eye - 0.5 * upper)

        def sweep(_, carry):
            cur_uppers, cur_lowers = carry
            new_uppers, new_lowers = [], []
            for upper, lower in zip(cur_uppers, cur_lowers):
                upper_hi, upper_lo = split(upper)
                lower_hi, lower_lo = split(lower)
                near = times(lower_hi, lower_lo, diag_rhs(upper_hi, upper_lo))
                near_hi, near_lo = split(near)
                stacked = times(
                    jnp.concatenate([upper_hi, lower_hi], axis=0),
                    jnp.concatenate([upper_lo, lower_lo], axis=0),
                    diag_rhs(near_hi, near_lo),
                )
                new_uppers.append(1.5 * upper - 0.5 * stacked[:K])
                new_lowers.append(1.5 * lower - 0.5 * stacked[K:])
            return tuple(new_uppers), tuple(new_lowers)

        uppers, lowers = lax.fori_loop(1, NSI - 1, sweep, (tuple(next_uppers), tuple(lowers)))

        mixings = []
        for pair in range(NR // 2):
            upper, lower = uppers[pair], lowers[pair]
            upper_hi, upper_lo = split(upper)
            lower_hi, lower_lo = split(lower)
            near = times(lower_hi, lower_lo, diag_rhs(upper_hi, upper_lo))
            lower = 1.5 * lower - 0.5 * times(lower_hi, lower_lo, diag_rhs(*split(near)))
            inv_root = lower / jnp.sqrt(scales[pair])
            half = halves_sum_exact(inv_root * drive_rows[pair])
            shift = jnp.sum(half * inv_root, axis=0, keepdims=True)
            transform = (K - 1.0) ** 0.5 * inv_root + shift
            mean = halves_sum_exact(transform) * (1.0 / K)
            mixings.append((1.0 / K + transform - mean).astype(bf16))
        mix_lo = jnp.concatenate(mixings[:2], axis=1)
        mix_hi = jnp.concatenate(mixings[2:], axis=1)

        first_col = pl.multiple_of(a * BLK, BLK)
        for group in range(K // 16):
            members = pl.ds(group * 16, 16)
            cells = jnp.concatenate(
                [
                    tile_ref[members, lev, pl.ds(first_col, BLK), :].reshape(256, ROWS)
                    for lev in range(LEV)
                ],
                axis=1,
            )
            z_ref[:, members, :] = dot(swap, cells).astype(bf16).reshape(16, 16, 2 * ROWS)

        def mix_column(c, _):
            cells = z_ref[c]
            low = jnp.concatenate([cells * m for m in group_masks[:4]], axis=0)
            high = jnp.concatenate([cells * m for m in group_masks[4:]], axis=0)
            o_ref[c] = (dot(mix_lo, low) + dot(mix_hi, high)).astype(bf16)
            return 0

        lax.fori_loop(0, BLK, mix_column, 0, unroll=4)

        for group in range(K // 16):
            members = pl.ds(group * 16, 16)
            cells = dot(swap, o_ref[:, members, :].reshape(256, 2 * ROWS)).astype(bf16)
            for lev in range(LEV):
                mixed_ref[members, lev, pl.ds(first_col, BLK), :] = cells[
                    :, lev * ROWS : (lev + 1) * ROWS
                ].reshape(16, BLK, ROWS)

        def start_exit(step, _):
            target, _source = peer(me, step)
            exit_copy(a, target, me).start()
            return 0

        lax.fori_loop(1, N_MEM, start_exit, 0)
        own_exit(a).start()
        return 0

    def exit_copy(a, target, owner):
        return pltpu.make_async_remote_copy(
            src_ref=mixed_ref.at[target, :, pl.ds(pl.multiple_of(a * BLK, BLK), BLK), :],
            dst_ref=out_ref.at[
                0, :, pl.ds(pl.multiple_of(owner * COLS + a * BLK, BLK), BLK), :
            ],
            send_sem=out_send.at[a, target],
            recv_sem=out_recv.at[a, owner],
            device_id=(target, gy),
            device_id_type=MESH,
        )

    def own_exit(a):
        return pltpu.make_async_copy(
            mixed_ref.at[me, :, pl.ds(pl.multiple_of(a * BLK, BLK), BLK), :],
            out_ref.at[0, :, pl.ds(pl.multiple_of(me * COLS + a * BLK, BLK), BLK), :],
            own_sem.at[1 + a],
        )

    lax.fori_loop(0, 2, band, 0)

    for a in range(2):
        own_exit(a).wait()

        def finish_exit(step, _):
            target, source = peer(me, step)
            exit_copy(a, target, source).wait()
            return 0

        lax.fori_loop(1, N_MEM, finish_exit, 0)


def local(state, obs_index, obs_count, obs_value, obs_var, radius):
    slots = obs_index[0]
    live = lax.broadcasted_iota(jnp.int32, (1, OBS), 1) < obs_count
    weight = jnp.where(live, 1.0 / obs_var[0], 0.0)
    meta = jnp.concatenate(
        [
            weight,
            obs_value[0],
            (slots // ROWS % COLS).astype(f32),
            (slots % ROWS).astype(f32),
            (slots // ROWS).astype(f32),
            jnp.broadcast_to(radius, (1, OBS)).astype(f32),
            jnp.zeros((2, OBS), f32),
        ],
        axis=0,
    )
    dma = pltpu.SemaphoreType.DMA
    return pl.pallas_call(
        kernel,
        out_shape=jax.ShapeDtypeStruct(state.shape, bf16),
        in_specs=[pl.BlockSpec(memory_space=pl.ANY), pl.BlockSpec(memory_space=pltpu.VMEM)],
        out_specs=pl.BlockSpec(memory_space=pl.ANY),
        scratch_shapes=[
            pltpu.VMEM((K, LEV, COLS, ROWS), bf16),
            pltpu.VMEM((K, LEV, COLS, ROWS), bf16),
            pltpu.VMEM((9, K, OBS), bf16),
            pltpu.VMEM((9, 8, OBS), f32),
            pltpu.VMEM((BLK, K, LEV * ROWS), bf16),
            pltpu.VMEM((BLK, K, LEV * ROWS), bf16),
            pltpu.VMEM((GRAM_ROWS, 2 * K), f32),
            dma((3,)),
            dma((N_MEM,)),
            dma((N_MEM,)),
            dma((8,)),
            dma((8,)),
            dma((8,)),
            dma((8,)),
            dma((2, N_MEM)),
            dma((2, N_MEM)),
        ],
        compiler_params=pltpu.CompilerParams(collective_id=0, has_side_effects=True),
    )(state, meta)


def solution(mesh):
    in_specs = (
        P("mem", None, None, "gy"),
        P("mem", "gy", None),
        P("mem", "gy"),
        P("mem", "gy", None),
        P("mem", "gy", None),
        P("mem", "gy"),
    )
    out_specs = P("mem", None, None, "gy")
    return jax.shard_map(local, mesh=mesh, in_specs=in_specs, out_specs=out_specs, check_vma=False)
```

```python
import functools

import jax
import jax.numpy as jnp
from jax import lax
from jax.experimental import pallas as pl
from jax.experimental.pallas import tpu as pltpu
from jax.sharding import PartitionSpec as P

K = 64
LEV = 2
ROWS = 128
COLS = 32
BLK = 16
OBS = 256
NSI = 10
N_MEM = 64
N_GY = 8
NR = ROWS // BLK
OWN = 4
GRAM_ROWS = NR * K + 16

MESH = pl.DeviceIdType.MESH
f32 = jnp.float32
bf16 = jnp.bfloat16

SIDES = [(dx, dy) for dx in (-1, 0, 1) for dy in (-1, 0, 1) if (dx, dy) != (0, 0)]


def split(x):
    hi = x.astype(bf16)
    lo = (x - hi.astype(f32)).astype(bf16)
    return hi, lo


def dot(a, b):
    return jnp.dot(a, b, preferred_element_type=f32)


def dot_nt(a, b):
    return lax.dot_general(a, b, (((1,), (1,)), ((), ())), preferred_element_type=f32)


def rem(a, b):
    return lax.rem(a, jnp.int32(b))


def peers_of(me):
    z, x, c = lax.div(me, jnp.int32(8)), rem(lax.div(me, jnp.int32(2)), 4), rem(me, 2)
    planes = [rem(z + d, 8) * 8 for d in range(8)]
    order = [0, 1, 7, 2, 6, 3, 5, 4]

    def each(fn):
        for dz in order[1:]:
            fn(planes[dz] + x * 2 + c, planes[8 - dz] + x * 2 + c)

        def row(r, _):
            dx, dc = lax.div(r, jnp.int32(2)), rem(r, 2)
            there = rem(x + dx, 4) * 2 + rem(c + dc, 2)
            back = rem(x + 4 - dx, 4) * 2 + rem(c + 2 - dc, 2)
            for dz in order:
                fn(planes[dz] + there, planes[(8 - dz) % 8] + back)
            return 0

        lax.fori_loop(1, 8, row, 0)

    return each


def kernel(
    state_ref, index_ref, count_ref, value_ref, var_ref, radius_ref, out_ref,
    tile_ref, mixed_ref, ens_ref, halo_ref, z_ref, o_ref, gram_ref,
    own_sem, in_send, in_recv, meta_send, meta_recv, ens_send, ens_recv, out_send, out_recv,
):
    me = lax.axis_index("mem")
    gy = lax.axis_index("gy")
    barrier = pltpu.get_barrier_semaphore()

    each_peer = peers_of(me)

    def greet(target, _source):
        pl.semaphore_signal(barrier, inc=1, device_id=(target, gy), device_id_type=MESH)

    each_peer(greet)
    for dx, dy in SIDES:
        if dy != 0:
            device = (rem(me + dx + N_MEM, N_MEM), rem(gy + dy + N_GY, N_GY))
            pl.semaphore_signal(barrier, inc=1, device_id=device, device_id_type=MESH)

    slots = index_ref[0]
    live = lax.broadcasted_iota(jnp.int32, (1, OBS), 1) < count_ref[0, 0]
    cell = lax.div(slots, jnp.int32(ROWS))
    meta = jnp.concatenate(
        [
            jnp.where(live, 1.0 / var_ref[0], 0.0),
            value_ref[0],
            rem(cell, COLS).astype(f32),
            rem(slots, ROWS).astype(f32),
            cell.astype(f32),
            jnp.zeros((3, OBS), f32),
        ],
        axis=0,
    )
    halo_ref[OWN] = meta
    radius = jnp.full((1, OBS), radius_ref[0, 0], jnp.int32).astype(f32)
    reach_sq = radius * radius
    pl.semaphore_wait(barrier, N_MEM - 1 + 6)

    def entry_copy(target, slot):
        return pltpu.make_async_remote_copy(
            src_ref=state_ref.at[0, :, pl.ds(pl.multiple_of(target * COLS, COLS), COLS), :],
            dst_ref=tile_ref.at[slot],
            send_sem=in_send.at[target],
            recv_sem=in_recv.at[slot],
            device_id=(target, gy),
            device_id_type=MESH,
        )

    def side_copy(src, dst, send, recv, index):
        dx, dy = SIDES[index]
        slot = (dx + 1) * 3 + dy + 1
        device = (rem(me - dx + N_MEM, N_MEM), rem(gy - dy + N_GY, N_GY))
        return pltpu.make_async_remote_copy(
            src_ref=src,
            dst_ref=dst.at[slot],
            send_sem=send.at[index],
            recv_sem=recv.at[index],
            device_id=device,
            device_id_type=MESH,
        )

    meta_copies = [side_copy(halo_ref.at[OWN], halo_ref, meta_send, meta_recv, i) for i in range(8)]
    for copy in meta_copies:
        copy.start()

    each_peer(lambda target, _source: entry_copy(target, me).start())
    own_in = pltpu.make_async_copy(
        state_ref.at[0, :, pl.ds(pl.multiple_of(me * COLS, COLS), COLS), :],
        tile_ref.at[me],
        own_sem.at[0],
    )
    own_in.start()
    own_in.wait()

    each_peer(lambda target, source: entry_copy(target, source).wait())

    pick_row = (
        lax.broadcasted_iota(jnp.int32, (ROWS, OBS), 0).astype(f32) == meta[3:4]
    ).astype(f32).astype(bf16)
    pick_col = lax.broadcasted_iota(jnp.int32, (LEV * COLS, OBS), 0).astype(f32) == meta[4:5]

    def observe(group, _):
        first = pl.multiple_of(group * 16, 16)
        cells = tile_ref[pl.ds(first, 16)].reshape(16 * LEV * COLS, ROWS)
        rows = dot(cells, pick_row).reshape(16, LEV * COLS, OBS)
        seen = jnp.sum(jnp.where(pick_col[None], rows, 0.0), axis=1)
        ens_ref[OWN, pl.ds(first, 16), :] = seen.astype(bf16)
        return 0

    lax.fori_loop(0, K // 16, observe, 0)

    ens_copies = [side_copy(ens_ref.at[OWN], ens_ref, ens_send, ens_recv, i) for i in range(8)]
    for copy in ens_copies:
        copy.start()
    for copy in meta_copies:
        copy.wait()
    for copy in ens_copies:
        copy.wait()

    left = lax.broadcasted_iota(jnp.int32, (K, 2 * K), 1) < K
    left_row = lax.broadcasted_iota(jnp.int32, (1, 2 * K), 1) < K
    lane = lax.broadcasted_iota(jnp.int32, (K, 2 * K), 1)
    eye = (lane % K == lax.broadcasted_iota(jnp.int32, (K, 2 * K), 0)).astype(f32)
    left_bf = jnp.where(left, 1.0, 0.0).astype(bf16)
    right_bf = jnp.where(left, 0.0, 1.0).astype(bf16)
    i_row = lax.broadcasted_iota(jnp.int32, (256, 256), 0)
    i_col = lax.broadcasted_iota(jnp.int32, (256, 256), 1)
    swap = jnp.where(
        (i_row // 16 == i_col % 16) & (i_row % 16 == i_col // 16), 1.0, 0.0
    ).astype(bf16)
    centre_r = lax.broadcasted_iota(jnp.int32, (NR, OBS), 0).astype(f32) * BLK + (BLK - 1) / 2.0
    row_group = lax.broadcasted_iota(jnp.int32, (K, 2 * ROWS), 1) % ROWS // BLK
    group_masks = [jnp.where(row_group == r, 1.0, 0.0).astype(bf16) for r in range(NR)]

    def halves_sum(x):
        total = jnp.sum(x, axis=1, keepdims=True)
        first = jnp.sum(jnp.where(left, x, 0.0), axis=1, keepdims=True)
        return jnp.where(left, first, total - first)

    def halves_sum_exact(x):
        first = jnp.sum(jnp.where(left, x, 0.0), axis=1, keepdims=True)
        second = jnp.sum(jnp.where(left, 0.0, x), axis=1, keepdims=True)
        return jnp.where(left, first, second)

    def weighted(slot, dx, dy, a):
        ens = ens_ref[slot].astype(f32)
        about = halo_ref[slot]
        centre = jnp.sum(ens, axis=0, keepdims=True) * (1.0 / K)
        spread = ens - centre
        innovation = about[1:2] - centre
        inside = (me + dx >= 0) & (me + dx < N_MEM) & (gy + dy >= 0) & (gy + dy < N_GY)
        weight = about[0:1] * jnp.where(inside, 1.0, 0.0)
        centre_c = (a * BLK).astype(f32) + (BLK - 1) / 2.0
        gap_c = (dx * COLS) * 1.0 + about[2:3] - centre_c
        gap_r = (dy * ROWS) * 1.0 + about[3:4] - centre_r
        taper = jnp.square(jnp.maximum(1.0 - (gap_c * gap_c + gap_r * gap_r) / reach_sq, 0.0))
        rho = taper * weight
        drive = jnp.concatenate([rho * innovation, jnp.zeros((8, OBS), f32)], axis=0)
        hi, lo = split(spread)
        return rho, spread, drive, jnp.concatenate([hi, lo], axis=0)

    def product(parts, both):
        hi, lo = split(jnp.concatenate(parts, axis=0))
        return dot_nt(hi, both) + dot_nt(lo, both)

    def band(a, _):
        dx = 2 * a - 1
        side = 6 * a + 1
        rho, spread, drive, both = weighted(OWN, 0, 0, a)
        gram_ref[...] = product([rho[r : r + 1] * spread for r in range(NR)] + [drive], both)
        rho, spread, drive, both = weighted(side, dx, 0, a)
        gram_ref[...] += product([rho[r : r + 1] * spread for r in range(NR)] + [drive], both)
        for dy, r in ((-1, 0), (1, NR - 1)):
            for slot, step in ((OWN + dy, 0), (side + dy, dx)):
                rho, spread, drive, both = weighted(slot, step, dy, a)
                part = product([rho[r : r + 1] * spread, drive], both)
                gram_ref[r * K : (r + 1) * K, :] += part[:K]
                gram_ref[NR * K :, :] += part[K:]

        def folded(block):
            return block + pltpu.roll(block, K, 1)

        drives = folded(gram_ref[NR * K :, :])
        uppers, lowers, scales, drive_rows = [], [], [], []
        for pair in range(NR // 2):
            r = 2 * pair
            first = folded(gram_ref[r * K : (r + 1) * K, :])
            second = folded(gram_ref[(r + 1) * K : (r + 2) * K, :])
            system = (K - 1.0) * eye + jnp.where(left, first, second)
            diagonal = jnp.sum(system * eye, axis=0, keepdims=True)
            trace_l = jnp.sum(jnp.where(left_row, diagonal, 0.0), axis=1, keepdims=True)
            trace_r = jnp.sum(jnp.where(left_row, 0.0, diagonal), axis=1, keepdims=True)
            scale = jnp.where(left_row, trace_l, trace_r)
            scales.append(scale)
            drive_rows.append(jnp.where(left_row, drives[r : r + 1], drives[r + 1 : r + 2]))
            uppers.append(system / scale)

        def diag_rhs(hi, lo):
            def blocks(x):
                return jnp.concatenate([x * left_bf, x * right_bf], axis=0)

            return blocks(hi), blocks(lo)

        def times(hi, lo, rhs):
            rhs_hi, rhs_lo = rhs
            return dot(
                jnp.concatenate([hi, lo], axis=1), jnp.concatenate([rhs_hi, rhs_hi], axis=0)
            ) + dot(hi, rhs_lo)

        next_uppers = []
        for upper in uppers:
            hi, lo = split(upper)
            next_uppers.append(1.5 * upper - 0.5 * times(hi, lo, diag_rhs(hi, lo)))
            lowers.append(1.5 * eye - 0.5 * upper)

        def sweep(_, carry):
            cur_uppers, cur_lowers = carry
            new_uppers, new_lowers = [], []
            for upper, lower in zip(cur_uppers, cur_lowers):
                upper_hi, upper_lo = split(upper)
                lower_hi, lower_lo = split(lower)
                near = times(lower_hi, lower_lo, diag_rhs(upper_hi, upper_lo))
                near_hi, near_lo = split(near)
                stacked = times(
                    jnp.concatenate([upper_hi, lower_hi], axis=0),
                    jnp.concatenate([upper_lo, lower_lo], axis=0),
                    diag_rhs(near_hi, near_lo),
                )
                new_uppers.append(1.5 * upper - 0.5 * stacked[:K])
                new_lowers.append(1.5 * lower - 0.5 * stacked[K:])
            return tuple(new_uppers), tuple(new_lowers)

        uppers, lowers = lax.fori_loop(1, NSI - 1, sweep, (tuple(next_uppers), tuple(lowers)))

        mixings = []
        for pair in range(NR // 2):
            upper, lower = uppers[pair], lowers[pair]
            upper_hi, upper_lo = split(upper)
            lower_hi, lower_lo = split(lower)
            near = times(lower_hi, lower_lo, diag_rhs(upper_hi, upper_lo))
            lower = 1.5 * lower - 0.5 * times(lower_hi, lower_lo, diag_rhs(*split(near)))
            inv_root = lower / jnp.sqrt(scales[pair])
            half = halves_sum_exact(inv_root * drive_rows[pair])
            shift = jnp.sum(half * inv_root, axis=0, keepdims=True)
            transform = (K - 1.0) ** 0.5 * inv_root + shift
            mean = halves_sum_exact(transform) * (1.0 / K)
            mixings.append((1.0 / K + transform - mean).astype(bf16))
        mix_lo = jnp.concatenate(mixings[:2], axis=1)
        mix_hi = jnp.concatenate(mixings[2:], axis=1)

        first_col = pl.multiple_of(a * BLK, BLK)
        for group in range(K // 16):
            members = pl.ds(group * 16, 16)
            cells = jnp.concatenate(
                [
                    tile_ref[members, lev, pl.ds(first_col, BLK), :].reshape(256, ROWS)
                    for lev in range(LEV)
                ],
                axis=1,
            )
            z_ref[:, members, :] = dot(swap, cells).astype(bf16).reshape(16, 16, 2 * ROWS)

        def mix_column(c, _):
            cells = z_ref[c]
            low = jnp.concatenate([cells * m for m in group_masks[:4]], axis=0)
            high = jnp.concatenate([cells * m for m in group_masks[4:]], axis=0)
            o_ref[c] = (dot(mix_lo, low) + dot(mix_hi, high)).astype(bf16)
            return 0

        lax.fori_loop(0, BLK, mix_column, 0, unroll=4)

        for group in range(K // 16):
            members = pl.ds(group * 16, 16)
            cells = dot(swap, o_ref[:, members, :].reshape(256, 2 * ROWS)).astype(bf16)
            for lev in range(LEV):
                mixed_ref[members, lev, pl.ds(first_col, BLK), :] = cells[
                    :, lev * ROWS : (lev + 1) * ROWS
                ].reshape(16, BLK, ROWS)

        each_peer(lambda target, _source: exit_copy(a, target, me).start())
        own_exit(a).start()
        return 0

    def exit_copy(a, target, owner):
        return pltpu.make_async_remote_copy(
            src_ref=mixed_ref.at[target, :, pl.ds(pl.multiple_of(a * BLK, BLK), BLK), :],
            dst_ref=out_ref.at[
                0, :, pl.ds(pl.multiple_of(owner * COLS + a * BLK, BLK), BLK), :
            ],
            send_sem=out_send.at[a, target],
            recv_sem=out_recv.at[a, owner],
            device_id=(target, gy),
            device_id_type=MESH,
        )

    def own_exit(a):
        return pltpu.make_async_copy(
            mixed_ref.at[me, :, pl.ds(pl.multiple_of(a * BLK, BLK), BLK), :],
            out_ref.at[0, :, pl.ds(pl.multiple_of(me * COLS + a * BLK, BLK), BLK), :],
            own_sem.at[1 + a],
        )

    lax.fori_loop(0, 2, band, 0)

    for a in range(2):
        own_exit(a).wait()

        each_peer(lambda target, source: exit_copy(a, target, source).wait())


def local(state, obs_index, obs_count, obs_value, obs_var, radius):
    dma = pltpu.SemaphoreType.DMA
    return pl.pallas_call(
        kernel,
        out_shape=jax.ShapeDtypeStruct(state.shape, bf16),
        in_specs=[
            pl.BlockSpec(memory_space=pl.ANY),
            pl.BlockSpec(memory_space=pltpu.VMEM),
            pl.BlockSpec(memory_space=pltpu.SMEM),
            pl.BlockSpec(memory_space=pltpu.VMEM),
            pl.BlockSpec(memory_space=pltpu.VMEM),
            pl.BlockSpec(memory_space=pltpu.SMEM),
        ],
        out_specs=pl.BlockSpec(memory_space=pl.ANY),
        scratch_shapes=[
            pltpu.VMEM((K, LEV, COLS, ROWS), bf16),
            pltpu.VMEM((K, LEV, COLS, ROWS), bf16),
            pltpu.VMEM((9, K, OBS), bf16),
            pltpu.VMEM((9, 8, OBS), f32),
            pltpu.VMEM((BLK, K, LEV * ROWS), bf16),
            pltpu.VMEM((BLK, K, LEV * ROWS), bf16),
            pltpu.VMEM((GRAM_ROWS, 2 * K), f32),
            dma((3,)),
            dma((N_MEM,)),
            dma((N_MEM,)),
            dma((8,)),
            dma((8,)),
            dma((8,)),
            dma((8,)),
            dma((2, N_MEM)),
            dma((2, N_MEM)),
        ],
        compiler_params=pltpu.CompilerParams(
            collective_id=0, has_side_effects=True, vmem_limit_bytes=24 * 2**20
        ),
    )(state, obs_index, obs_count, obs_value, obs_var, radius)


def solution(mesh):
    in_specs = (
        P("mem", None, None, "gy"),
        P("mem", "gy", None),
        P("mem", "gy"),
        P("mem", "gy", None),
        P("mem", "gy", None),
        P("mem", "gy"),
    )
    out_specs = P("mem", None, None, "gy")
    return jax.shard_map(local, mesh=mesh, in_specs=in_specs, out_specs=out_specs, check_vma=False)
```

```python
import functools

import jax
import jax.numpy as jnp
from jax import lax
from jax.experimental import pallas as pl
from jax.experimental.pallas import tpu as pltpu
from jax.sharding import PartitionSpec as P

K = 64
LEV = 2
ROWS = 128
COLS = 32
BLK = 16
OBS = 256
NSI = 10
N_MEM = 64
N_GY = 8
NR = ROWS // BLK
OWN = 4
BULK = (3, 5, 8)
GRAM_ROWS = NR * K + 16

MESH = pl.DeviceIdType.MESH
f32 = jnp.float32
bf16 = jnp.bfloat16

SIDES = [(dx, dy) for dx in (-1, 0, 1) for dy in (-1, 0, 1) if (dx, dy) != (0, 0)]


def split(x):
    hi = x.astype(bf16)
    lo = (x - hi.astype(f32)).astype(bf16)
    return hi, lo


def dot(a, b):
    return jnp.dot(a, b, preferred_element_type=f32)


def dot_nt(a, b):
    return lax.dot_general(a, b, (((1,), (1,)), ((), ())), preferred_element_type=f32)


def rem(a, b):
    return lax.rem(a, jnp.int32(b))


def peers_of(me):
    z, x, c = lax.div(me, jnp.int32(8)), rem(lax.div(me, jnp.int32(2)), 4), rem(me, 2)
    planes = [rem(z + d, 8) * 8 for d in range(8)]
    order = [0, 1, 7, 2, 6, 3, 5, 4]

    def each(fn, first=0, last=8):
        if first == 0:
            for dz in order[1:]:
                fn(planes[dz] + x * 2 + c, planes[8 - dz] + x * 2 + c)

        def row(r, _):
            dx, dc = lax.div(r, jnp.int32(2)), rem(r, 2)
            there = rem(x + dx, 4) * 2 + rem(c + dc, 2)
            back = rem(x + 4 - dx, 4) * 2 + rem(c + 2 - dc, 2)
            for dz in order:
                fn(planes[dz] + there, planes[(8 - dz) % 8] + back)
            return 0

        lax.fori_loop(max(first, 1), last, row, 0)

    return each


def kernel(
    state_ref, index_ref, count_ref, value_ref, var_ref, radius_ref, out_ref,
    index_all, seen_ref, raw_ref,
    tile_ref, mixed_ref, ens_ref, halo_ref, z_ref, o_ref, gram_ref, mix_ref,
    own_sem, index_send, index_recv, seen_send, seen_recv, in_send, in_recv, meta_send, meta_recv, ens_send, ens_recv, out_send, out_recv,
):
    me = lax.axis_index("mem")
    gy = lax.axis_index("gy")
    barrier = pltpu.get_barrier_semaphore()

    each_peer = peers_of(me)

    def greet(target, _source):
        pl.semaphore_signal(barrier, inc=1, device_id=(target, gy), device_id_type=MESH)

    each_peer(greet)
    for dx, dy in SIDES:
        if dy != 0:
            device = (rem(me + dx + N_MEM, N_MEM), rem(gy + dy + N_GY, N_GY))
            pl.semaphore_signal(barrier, inc=1, device_id=device, device_id_type=MESH)

    slots = index_ref[0]
    live = lax.broadcasted_iota(jnp.int32, (1, OBS), 1) < count_ref[...]
    cell = lax.div(slots, jnp.int32(ROWS))
    meta = jnp.concatenate(
        [
            jnp.where(live, 1.0 / var_ref[0], 0.0),
            value_ref[0],
            rem(cell, COLS).astype(f32),
            rem(slots, ROWS).astype(f32),
            cell.astype(f32),
            jnp.zeros((3, OBS), f32),
        ],
        axis=0,
    )
    halo_ref[OWN] = meta
    radius = jnp.broadcast_to(radius_ref[...], (1, OBS)).astype(f32)
    reach_sq = radius * radius
    pl.semaphore_wait(barrier, N_MEM - 1 + 6)

    def entry_copy(target, slot):
        return pltpu.make_async_remote_copy(
            src_ref=state_ref.at[0, :, pl.ds(pl.multiple_of(target * COLS, COLS), COLS), :],
            dst_ref=tile_ref.at[slot],
            send_sem=in_send.at[target],
            recv_sem=in_recv.at[slot],
            device_id=(target, gy),
            device_id_type=MESH,
        )

    def side_copy(src, dst, send, recv, index):
        dx, dy = SIDES[index]
        slot = (dx + 1) * 3 + dy + 1
        device = (rem(me - dx + N_MEM, N_MEM), rem(gy - dy + N_GY, N_GY))
        return pltpu.make_async_remote_copy(
            src_ref=src,
            dst_ref=dst.at[slot],
            send_sem=send.at[index],
            recv_sem=recv.at[index],
            device_id=device,
            device_id_type=MESH,
        )

    def index_copy(target, slot):
        return pltpu.make_async_remote_copy(
            src_ref=index_ref.at[0],
            dst_ref=index_all.at[slot],
            send_sem=index_send.at[target],
            recv_sem=index_recv.at[slot],
            device_id=(target, gy),
            device_id_type=MESH,
        )

    def seen_copy(target, slot):
        return pltpu.make_async_remote_copy(
            src_ref=seen_ref.at[target],
            dst_ref=raw_ref.at[slot],
            send_sem=seen_send.at[target],
            recv_sem=seen_recv.at[slot],
            device_id=(target, gy),
            device_id_type=MESH,
        )

    def start_entry(target, _source):
        entry_copy(target, me).start()

    each_peer(lambda target, _source: index_copy(target, me).start())
    meta_copies = [side_copy(halo_ref.at[OWN], halo_ref, meta_send, meta_recv, i) for i in range(8)]
    for copy in meta_copies:
        copy.start()
    each_peer(start_entry, 0, BULK[0])
    own_in = pltpu.make_async_copy(
        state_ref.at[0, :, pl.ds(pl.multiple_of(me * COLS, COLS), COLS), :],
        tile_ref.at[me],
        own_sem.at[0],
    )
    own_in.start()
    own_in.wait()
    index_all[me] = index_ref[0]
    each_peer(lambda target, source: index_copy(target, source).wait())

    row_iota = lax.broadcasted_iota(jnp.int32, (ROWS, OBS), 0)
    cell_iota = lax.broadcasted_iota(jnp.int32, (LEV * COLS, OBS), 0)

    def observe(tile, _):
        wanted = index_all[tile]
        pick_row = jnp.where(row_iota == (wanted & (ROWS - 1)), 1.0, 0.0).astype(bf16)
        cells = state_ref[0, :, pl.ds(pl.multiple_of(tile * COLS, COLS), COLS), :]
        rows = dot(cells.reshape(LEV * COLS, ROWS), pick_row)
        picked = jnp.where(cell_iota == (wanted >> 7), rows, 0.0)
        seen_ref[tile] = jnp.sum(picked, axis=0, keepdims=True)
        return 0

    lax.fori_loop(0, N_MEM, observe, 0, unroll=8)
    raw_ref[me] = seen_ref[me]
    each_peer(lambda target, _source: seen_copy(target, me).start())
    each_peer(start_entry, *BULK[:2])
    each_peer(lambda target, source: seen_copy(target, source).wait())

    ens_ref[OWN] = raw_ref[:, 0, :].astype(bf16)
    ens_copies = [side_copy(ens_ref.at[OWN], ens_ref, ens_send, ens_recv, i) for i in range(8)]
    for copy in ens_copies:
        copy.start()
    each_peer(start_entry, *BULK[1:])

    left = lax.broadcasted_iota(jnp.int32, (K, 2 * K), 1) < K
    left_row = lax.broadcasted_iota(jnp.int32, (1, 2 * K), 1) < K
    lane = lax.broadcasted_iota(jnp.int32, (K, 2 * K), 1)
    eye = (lane % K == lax.broadcasted_iota(jnp.int32, (K, 2 * K), 0)).astype(f32)
    left_bf = jnp.where(left, 1.0, 0.0).astype(bf16)
    right_bf = jnp.where(left, 0.0, 1.0).astype(bf16)
    i_row = lax.broadcasted_iota(jnp.int32, (256, 256), 0)
    i_col = lax.broadcasted_iota(jnp.int32, (256, 256), 1)
    swap = jnp.where(
        (i_row // 16 == i_col % 16) & (i_row % 16 == i_col // 16), 1.0, 0.0
    ).astype(bf16)
    centre_r = lax.broadcasted_iota(jnp.int32, (NR, OBS), 0).astype(f32) * BLK + (BLK - 1) / 2.0
    row_group = lax.broadcasted_iota(jnp.int32, (K, 2 * ROWS), 1) % ROWS // BLK
    group_masks = [jnp.where(row_group == r, 1.0, 0.0).astype(bf16) for r in range(NR)]

    def halves_sum(x):
        total = jnp.sum(x, axis=1, keepdims=True)
        first = jnp.sum(jnp.where(left, x, 0.0), axis=1, keepdims=True)
        return jnp.where(left, first, total - first)

    def halves_sum_exact(x):
        first = jnp.sum(jnp.where(left, x, 0.0), axis=1, keepdims=True)
        second = jnp.sum(jnp.where(left, 0.0, x), axis=1, keepdims=True)
        return jnp.where(left, first, second)

    def weighted(slot, dx, dy, a):
        ens = ens_ref[slot].astype(f32)
        about = halo_ref[slot]
        centre = jnp.sum(ens, axis=0, keepdims=True) * (1.0 / K)
        spread = ens - centre
        innovation = about[1:2] - centre
        inside = (me + dx >= 0) & (me + dx < N_MEM) & (gy + dy >= 0) & (gy + dy < N_GY)
        weight = about[0:1] * jnp.where(inside, 1.0, 0.0)
        centre_c = a * BLK + (BLK - 1) / 2.0
        gap_c = (dx * COLS) * 1.0 + about[2:3] - centre_c
        gap_r = (dy * ROWS) * 1.0 + about[3:4] - centre_r
        taper = jnp.square(jnp.maximum(1.0 - (gap_c * gap_c + gap_r * gap_r) / reach_sq, 0.0))
        rho = taper * weight
        drive = jnp.concatenate([rho * innovation, jnp.zeros((8, OBS), f32)], axis=0)
        hi, lo = split(spread)
        return rho, spread, drive, jnp.concatenate([hi, lo], axis=0)

    def product(parts, both):
        hi, lo = split(jnp.concatenate(parts, axis=0))
        return dot_nt(hi, both) + dot_nt(lo, both)

    for a in range(2):
        rho, spread, drive, both = weighted(OWN, 0, 0, a)
        gram_ref[a] = product([rho[r : r + 1] * spread for r in range(NR)] + [drive], both)
    for copy in meta_copies:
        copy.wait()
    for copy in ens_copies:
        copy.wait()

    def folded(block):
        return block + pltpu.roll(block, K, 1)

    uppers, lowers, scales, drive_rows = [], [], [], []
    for a in range(2):
        dx = 2 * a - 1
        side = 6 * a + 1
        rho, spread, drive, both = weighted(side, dx, 0, a)
        gram_ref[a] += product([rho[r : r + 1] * spread for r in range(NR)] + [drive], both)
        for dy, r in ((-1, 0), (1, NR - 1)):
            for slot, step in ((OWN + dy, 0), (side + dy, dx)):
                rho, spread, drive, both = weighted(slot, step, dy, a)
                part = product([rho[r : r + 1] * spread, drive], both)
                gram_ref[a, r * K : (r + 1) * K, :] += part[:K]
                gram_ref[a, NR * K :, :] += part[K:]

        drives = folded(gram_ref[a, NR * K :, :])
        for pair in range(NR // 2):
            r = 2 * pair
            first = folded(gram_ref[a, r * K : (r + 1) * K, :])
            second = folded(gram_ref[a, (r + 1) * K : (r + 2) * K, :])
            system = (K - 1.0) * eye + jnp.where(left, first, second)
            diagonal = jnp.sum(system * eye, axis=0, keepdims=True)
            trace_l = jnp.sum(jnp.where(left_row, diagonal, 0.0), axis=1, keepdims=True)
            trace_r = jnp.sum(jnp.where(left_row, 0.0, diagonal), axis=1, keepdims=True)
            scale = jnp.where(left_row, trace_l, trace_r)
            scales.append(scale)
            drive_rows.append(jnp.where(left_row, drives[r : r + 1], drives[r + 1 : r + 2]))
            uppers.append(system / scale)

    def diag_rhs(hi, lo):
        def blocks(x):
            return jnp.concatenate([x * left_bf, x * right_bf], axis=0)

        return blocks(hi), blocks(lo)

    def times(hi, lo, rhs):
        rhs_hi, rhs_lo = rhs
        return dot(
            jnp.concatenate([hi, lo], axis=1), jnp.concatenate([rhs_hi, rhs_hi], axis=0)
        ) + dot(hi, rhs_lo)

    next_uppers = []
    for upper in uppers:
        hi, lo = split(upper)
        next_uppers.append(1.5 * upper - 0.5 * times(hi, lo, diag_rhs(hi, lo)))
        lowers.append(1.5 * eye - 0.5 * upper)

    def sweep(_, carry):
        cur_uppers, cur_lowers = carry
        new_uppers, new_lowers = [], []
        for upper, lower in zip(cur_uppers, cur_lowers):
            upper_hi, upper_lo = split(upper)
            lower_hi, lower_lo = split(lower)
            near = times(lower_hi, lower_lo, diag_rhs(upper_hi, upper_lo))
            near_hi, near_lo = split(near)
            stacked = times(
                jnp.concatenate([upper_hi, lower_hi], axis=0),
                jnp.concatenate([upper_lo, lower_lo], axis=0),
                diag_rhs(near_hi, near_lo),
            )
            new_uppers.append(1.5 * upper - 0.5 * stacked[:K])
            new_lowers.append(1.5 * lower - 0.5 * stacked[K:])
        return tuple(new_uppers), tuple(new_lowers)

    uppers, lowers = lax.fori_loop(1, NSI - 1, sweep, (tuple(next_uppers), tuple(lowers)))

    mixings = []
    for pair in range(NR):
        upper, lower = uppers[pair], lowers[pair]
        upper_hi, upper_lo = split(upper)
        lower_hi, lower_lo = split(lower)
        near = times(lower_hi, lower_lo, diag_rhs(upper_hi, upper_lo))
        lower = 1.5 * lower - 0.5 * times(lower_hi, lower_lo, diag_rhs(*split(near)))
        inv_root = lower / jnp.sqrt(scales[pair])
        half = halves_sum_exact(inv_root * drive_rows[pair])
        shift = jnp.sum(half * inv_root, axis=0, keepdims=True)
        transform = (K - 1.0) ** 0.5 * inv_root + shift
        mean = halves_sum_exact(transform) * (1.0 / K)
        mixings.append((1.0 / K + transform - mean).astype(bf16))
    for a in range(2):
        for half in range(2):
            first = 4 * a + 2 * half
            mix_ref[a, half] = jnp.concatenate(mixings[first : first + 2], axis=1)

    each_peer(lambda target, source: entry_copy(target, source).wait())

    def band(a, _):
        mix_lo = mix_ref[a, 0]
        mix_hi = mix_ref[a, 1]

        first_col = pl.multiple_of(a * BLK, BLK)
        for group in range(K // 16):
            members = pl.ds(group * 16, 16)
            cells = jnp.concatenate(
                [
                    tile_ref[members, lev, pl.ds(first_col, BLK), :].reshape(256, ROWS)
                    for lev in range(LEV)
                ],
                axis=1,
            )
            z_ref[:, members, :] = dot(swap, cells).astype(bf16).reshape(16, 16, 2 * ROWS)

        def mix_column(c, _):
            cells = z_ref[c]
            low = jnp.concatenate([cells * m for m in group_masks[:4]], axis=0)
            high = jnp.concatenate([cells * m for m in group_masks[4:]], axis=0)
            o_ref[c] = (dot(mix_lo, low) + dot(mix_hi, high)).astype(bf16)
            return 0

        lax.fori_loop(0, BLK, mix_column, 0, unroll=4)

        for group in range(K // 16):
            members = pl.ds(group * 16, 16)
            cells = dot(swap, o_ref[:, members, :].reshape(256, 2 * ROWS)).astype(bf16)
            for lev in range(LEV):
                mixed_ref[members, lev, pl.ds(first_col, BLK), :] = cells[
                    :, lev * ROWS : (lev + 1) * ROWS
                ].reshape(16, BLK, ROWS)

        each_peer(lambda target, _source: exit_copy(a, target, me).start())
        own_exit(a).start()
        return 0

    def exit_copy(a, target, owner):
        return pltpu.make_async_remote_copy(
            src_ref=mixed_ref.at[target, :, pl.ds(pl.multiple_of(a * BLK, BLK), BLK), :],
            dst_ref=out_ref.at[
                0, :, pl.ds(pl.multiple_of(owner * COLS + a * BLK, BLK), BLK), :
            ],
            send_sem=out_send.at[a, target],
            recv_sem=out_recv.at[a, owner],
            device_id=(target, gy),
            device_id_type=MESH,
        )

    def own_exit(a):
        return pltpu.make_async_copy(
            mixed_ref.at[me, :, pl.ds(pl.multiple_of(a * BLK, BLK), BLK), :],
            out_ref.at[0, :, pl.ds(pl.multiple_of(me * COLS + a * BLK, BLK), BLK), :],
            own_sem.at[1 + a],
        )

    lax.fori_loop(0, 2, band, 0)

    for a in range(2):
        own_exit(a).wait()

        each_peer(lambda target, source: exit_copy(a, target, source).wait())


def local(state, obs_index, obs_count, obs_value, obs_var, radius):
    dma = pltpu.SemaphoreType.DMA
    return pl.pallas_call(
        kernel,
        out_shape=jax.ShapeDtypeStruct(state.shape, bf16),
        in_specs=[pl.BlockSpec(memory_space=pltpu.VMEM)] * 6,
        out_specs=pl.BlockSpec(memory_space=pl.ANY),
        scratch_shapes=[
            pltpu.VMEM((N_MEM, 1, OBS), jnp.int32),
            pltpu.VMEM((N_MEM, 1, OBS), f32),
            pltpu.VMEM((N_MEM, 1, OBS), f32),
            pltpu.VMEM((K, LEV, COLS, ROWS), bf16),
            pltpu.VMEM((K, LEV, COLS, ROWS), bf16),
            pltpu.VMEM((9, K, OBS), bf16),
            pltpu.VMEM((9, 8, OBS), f32),
            pltpu.VMEM((BLK, K, LEV * ROWS), bf16),
            pltpu.VMEM((BLK, K, LEV * ROWS), bf16),
            pltpu.VMEM((2, GRAM_ROWS, 2 * K), f32),
            pltpu.VMEM((2, 2, K, 4 * K), bf16),
            dma((3,)),
            dma((N_MEM,)),
            dma((N_MEM,)),
            dma((N_MEM,)),
            dma((N_MEM,)),
            dma((N_MEM,)),
            dma((N_MEM,)),
            dma((8,)),
            dma((8,)),
            dma((8,)),
            dma((8,)),
            dma((2, N_MEM)),
            dma((2, N_MEM)),
        ],
        compiler_params=pltpu.CompilerParams(
            collective_id=0, has_side_effects=True, vmem_limit_bytes=24 * 2**20
        ),
    )(state, obs_index, obs_count, obs_value, obs_var, radius)


def solution(mesh):
    in_specs = (
        P("mem", None, None, "gy"),
        P("mem", "gy", None),
        P("mem", "gy"),
        P("mem", "gy", None),
        P("mem", "gy", None),
        P("mem", "gy"),
    )
    out_specs = P("mem", None, None, "gy")
    return jax.shard_map(local, mesh=mesh, in_specs=in_specs, out_specs=out_specs, check_vma=False)
```

```python
import functools

import jax
import jax.numpy as jnp
from jax import lax
from jax.experimental import pallas as pl
from jax.experimental.pallas import tpu as pltpu
from jax.sharding import PartitionSpec as P

K = 64
LEV = 2
ROWS = 128
COLS = 32
BLK = 16
OBS = 256
NSI = 10
N_MEM = 64
N_GY = 8
NR = ROWS // BLK
OWN = 4
BULK = (3, 5, 8)
GRAM_ROWS = NR * K + 16

MESH = pl.DeviceIdType.MESH
f32 = jnp.float32
bf16 = jnp.bfloat16

SIDES = [(dx, dy) for dx in (-1, 0, 1) for dy in (-1, 0, 1) if (dx, dy) != (0, 0)]


def split(x):
    hi = x.astype(bf16)
    lo = (x - hi.astype(f32)).astype(bf16)
    return hi, lo


def dot(a, b):
    return jnp.dot(a, b, preferred_element_type=f32)


def dot_nt(a, b):
    return lax.dot_general(a, b, (((1,), (1,)), ((), ())), preferred_element_type=f32)


def rem(a, b):
    return lax.rem(a, jnp.int32(b))


def peers_of(me):
    z, x, c = lax.div(me, jnp.int32(8)), rem(lax.div(me, jnp.int32(2)), 4), rem(me, 2)
    planes = [rem(z + d, 8) * 8 for d in range(8)]
    order = [0, 1, 7, 2, 6, 3, 5, 4]

    def each(fn, first=0, last=8):
        if first == 0:
            for dz in order[1:]:
                fn(planes[dz] + x * 2 + c, planes[8 - dz] + x * 2 + c)

        def row(r, _):
            dx, dc = lax.div(r, jnp.int32(2)), rem(r, 2)
            there = rem(x + dx, 4) * 2 + rem(c + dc, 2)
            back = rem(x + 4 - dx, 4) * 2 + rem(c + 2 - dc, 2)
            for dz in order:
                fn(planes[dz] + there, planes[(8 - dz) % 8] + back)
            return 0

        lax.fori_loop(max(first, 1), last, row, 0)

    return each


def kernel(
    state_ref, index_ref, count_ref, value_ref, var_ref, radius_ref, out_ref,
    index_all, seen_ref, raw_ref,
    tile_ref, mixed_ref, ens_ref, halo_ref, z_ref, o_ref, gram_ref, mix_ref,
    own_sem, index_send, index_recv, seen_send, seen_recv, in_send, in_recv, meta_send, meta_recv, ens_send, ens_recv, out_send, out_recv,
):
    me = lax.axis_index("mem")
    gy = lax.axis_index("gy")
    barrier = pltpu.get_barrier_semaphore()

    each_peer = peers_of(me)

    def greet(target, _source):
        pl.semaphore_signal(barrier, inc=1, device_id=(target, gy), device_id_type=MESH)

    each_peer(greet)
    for dx, dy in SIDES:
        if dy != 0:
            device = (rem(me + dx + N_MEM, N_MEM), rem(gy + dy + N_GY, N_GY))
            pl.semaphore_signal(barrier, inc=1, device_id=device, device_id_type=MESH)

    slots = index_ref[0]
    live = lax.broadcasted_iota(jnp.int32, (1, OBS), 1) < count_ref[...]
    cell = lax.div(slots, jnp.int32(ROWS))
    meta = jnp.concatenate(
        [
            jnp.where(live, 1.0 / var_ref[0], 0.0),
            value_ref[0],
            rem(cell, COLS).astype(f32),
            rem(slots, ROWS).astype(f32),
            cell.astype(f32),
            jnp.zeros((3, OBS), f32),
        ],
        axis=0,
    )
    halo_ref[OWN] = meta
    radius = jnp.broadcast_to(radius_ref[...], (1, OBS)).astype(f32)
    reach_sq = radius * radius
    pl.semaphore_wait(barrier, N_MEM - 1 + 6)

    def entry_copy(target, slot):
        return pltpu.make_async_remote_copy(
            src_ref=state_ref.at[0, :, pl.ds(pl.multiple_of(target * COLS, COLS), COLS), :],
            dst_ref=tile_ref.at[slot],
            send_sem=in_send.at[target],
            recv_sem=in_recv.at[slot],
            device_id=(target, gy),
            device_id_type=MESH,
        )

    def side_copy(src, dst, send, recv, index):
        dx, dy = SIDES[index]
        slot = (dx + 1) * 3 + dy + 1
        device = (rem(me - dx + N_MEM, N_MEM), rem(gy - dy + N_GY, N_GY))
        return pltpu.make_async_remote_copy(
            src_ref=src,
            dst_ref=dst.at[slot],
            send_sem=send.at[index],
            recv_sem=recv.at[index],
            device_id=device,
            device_id_type=MESH,
        )

    def index_copy(target, slot):
        return pltpu.make_async_remote_copy(
            src_ref=index_ref.at[0],
            dst_ref=index_all.at[slot],
            send_sem=index_send.at[target],
            recv_sem=index_recv.at[slot],
            device_id=(target, gy),
            device_id_type=MESH,
        )

    def seen_copy(target, slot):
        return pltpu.make_async_remote_copy(
            src_ref=seen_ref.at[target],
            dst_ref=raw_ref.at[slot],
            send_sem=seen_send.at[target],
            recv_sem=seen_recv.at[slot],
            device_id=(target, gy),
            device_id_type=MESH,
        )

    def start_entry(target, _source):
        entry_copy(target, me).start()

    each_peer(lambda target, _source: index_copy(target, me).start())
    meta_copies = [side_copy(halo_ref.at[OWN], halo_ref, meta_send, meta_recv, i) for i in range(8)]
    for copy in meta_copies:
        copy.start()
    each_peer(start_entry, 0, BULK[0])
    own_in = pltpu.make_async_copy(
        state_ref.at[0, :, pl.ds(pl.multiple_of(me * COLS, COLS), COLS), :],
        tile_ref.at[me],
        own_sem.at[0],
    )
    own_in.start()
    own_in.wait()
    index_all[me] = index_ref[0]
    each_peer(lambda target, source: index_copy(target, source).wait())

    row_iota = lax.broadcasted_iota(jnp.int32, (ROWS, OBS), 0)
    cell_iota = lax.broadcasted_iota(jnp.int32, (LEV * COLS, OBS), 0)

    def observe(tile, _):
        wanted = index_all[tile]
        pick_row = jnp.where(row_iota == (wanted & (ROWS - 1)), 1.0, 0.0).astype(bf16)
        cells = state_ref[0, :, pl.ds(pl.multiple_of(tile * COLS, COLS), COLS), :]
        rows = dot(cells.reshape(LEV * COLS, ROWS), pick_row)
        picked = jnp.where(cell_iota == (wanted >> 7), rows, 0.0)
        seen_ref[tile] = jnp.sum(picked, axis=0, keepdims=True)
        return 0

    lax.fori_loop(0, N_MEM, observe, 0, unroll=8)
    raw_ref[me] = seen_ref[me]
    each_peer(lambda target, _source: seen_copy(target, me).start())
    each_peer(start_entry, *BULK[:2])
    each_peer(lambda target, source: seen_copy(target, source).wait())

    ens_ref[OWN] = raw_ref[:, 0, :].astype(bf16)
    ens_copies = [side_copy(ens_ref.at[OWN], ens_ref, ens_send, ens_recv, i) for i in range(8)]
    for copy in ens_copies:
        copy.start()
    each_peer(start_entry, *BULK[1:])

    left = lax.broadcasted_iota(jnp.int32, (K, 2 * K), 1) < K
    left_row = lax.broadcasted_iota(jnp.int32, (1, 2 * K), 1) < K
    lane = lax.broadcasted_iota(jnp.int32, (K, 2 * K), 1)
    eye = (lane % K == lax.broadcasted_iota(jnp.int32, (K, 2 * K), 0)).astype(f32)
    left_bf = jnp.where(left, 1.0, 0.0).astype(bf16)
    right_bf = jnp.where(left, 0.0, 1.0).astype(bf16)
    i_row = lax.broadcasted_iota(jnp.int32, (256, 256), 0)
    i_col = lax.broadcasted_iota(jnp.int32, (256, 256), 1)
    swap = jnp.where(
        (i_row // 16 == i_col % 16) & (i_row % 16 == i_col // 16), 1.0, 0.0
    ).astype(bf16)
    centre_r = lax.broadcasted_iota(jnp.int32, (NR, OBS), 0).astype(f32) * BLK + (BLK - 1) / 2.0
    row_group = lax.broadcasted_iota(jnp.int32, (K, 2 * ROWS), 1) % ROWS // BLK
    group_masks = [jnp.where(row_group == r, 1.0, 0.0).astype(bf16) for r in range(NR)]

    def halves_sum(x):
        total = jnp.sum(x, axis=1, keepdims=True)
        first = jnp.sum(jnp.where(left, x, 0.0), axis=1, keepdims=True)
        return jnp.where(left, first, total - first)

    def halves_sum_exact(x):
        first = jnp.sum(jnp.where(left, x, 0.0), axis=1, keepdims=True)
        second = jnp.sum(jnp.where(left, 0.0, x), axis=1, keepdims=True)
        return jnp.where(left, first, second)

    def weighted(slot, dx, dy, a):
        ens = ens_ref[slot].astype(f32)
        about = halo_ref[slot]
        centre = jnp.sum(ens, axis=0, keepdims=True) * (1.0 / K)
        spread = ens - centre
        innovation = about[1:2] - centre
        inside = (me + dx >= 0) & (me + dx < N_MEM) & (gy + dy >= 0) & (gy + dy < N_GY)
        weight = about[0:1] * jnp.where(inside, 1.0, 0.0)
        centre_c = a * BLK + (BLK - 1) / 2.0
        gap_c = (dx * COLS) * 1.0 + about[2:3] - centre_c
        gap_r = (dy * ROWS) * 1.0 + about[3:4] - centre_r
        taper = jnp.square(jnp.maximum(1.0 - (gap_c * gap_c + gap_r * gap_r) / reach_sq, 0.0))
        rho = taper * weight
        drive = jnp.concatenate([rho * innovation, jnp.zeros((8, OBS), f32)], axis=0)
        hi, lo = split(spread)
        return rho, spread, drive, jnp.concatenate([hi, lo], axis=0)

    def product(parts, both):
        hi, lo = split(jnp.concatenate(parts, axis=0))
        return dot_nt(hi, both) + dot_nt(lo, both)

    for a in range(2):
        rho, spread, drive, both = weighted(OWN, 0, 0, a)
        gram_ref[a] = product([rho[r : r + 1] * spread for r in range(NR)] + [drive], both)
    for copy in meta_copies:
        copy.wait()
    for copy in ens_copies:
        copy.wait()

    def folded(block):
        return block + pltpu.roll(block, K, 1)

    def diag_rhs(hi, lo):
        return jnp.concatenate(
            [
                jnp.concatenate([hi * left_bf, hi * right_bf], axis=0),
                jnp.concatenate([lo * left_bf, lo * right_bf], axis=0),
            ],
            axis=1,
        )

    def times(parts, rhs):
        out = dot(jnp.concatenate([x for part in parts for x in part], axis=0), rhs)
        sides = out[:, : 2 * K] + out[:, 2 * K :]
        return [sides[2 * i * K : (2 * i + 1) * K] + sides[(2 * i + 1) * K : 2 * (i + 1) * K] for i in range(len(parts))]

    def solve(a):
        uppers, lowers, scales, drive_rows = [], [], [], []
        dx = 2 * a - 1
        side = 6 * a + 1
        rho, spread, drive, both = weighted(side, dx, 0, a)
        gram_ref[a] += product([rho[r : r + 1] * spread for r in range(NR)] + [drive], both)
        for dy, r in ((-1, 0), (1, NR - 1)):
            for slot, step in ((OWN + dy, 0), (side + dy, dx)):
                rho, spread, drive, both = weighted(slot, step, dy, a)
                part = product([rho[r : r + 1] * spread, drive], both)
                gram_ref[a, r * K : (r + 1) * K, :] += part[:K]
                gram_ref[a, NR * K :, :] += part[K:]

        drives = folded(gram_ref[a, NR * K :, :])
        for pair in range(NR // 2):
            r = 2 * pair
            first = folded(gram_ref[a, r * K : (r + 1) * K, :])
            second = folded(gram_ref[a, (r + 1) * K : (r + 2) * K, :])
            system = (K - 1.0) * eye + jnp.where(left, first, second)
            diagonal = jnp.sum(system * eye, axis=0, keepdims=True)
            trace_l = jnp.sum(jnp.where(left_row, diagonal, 0.0), axis=1, keepdims=True)
            trace_r = jnp.sum(jnp.where(left_row, 0.0, diagonal), axis=1, keepdims=True)
            scale = jnp.where(left_row, trace_l, trace_r)
            scales.append(scale)
            drive_rows.append(jnp.where(left_row, drives[r : r + 1], drives[r + 1 : r + 2]))
            uppers.append(system / scale)

        next_uppers = []
        for upper in uppers:
            halves = split(upper)
            next_uppers.append(1.5 * upper - 0.5 * times([halves], diag_rhs(*halves))[0])
            lowers.append(1.5 * eye - 0.5 * upper)

        def sweep(_, carry):
            cur_uppers, cur_lowers = carry
            upper_halves = [split(upper) for upper in cur_uppers]
            lower_halves = [split(lower) for lower in cur_lowers]
            nears = [times([lo], diag_rhs(*up))[0] for lo, up in zip(lower_halves, upper_halves)]
            steps = [
                times([up, lo], diag_rhs(*split(near)))
                for up, lo, near in zip(upper_halves, lower_halves, nears)
            ]
            new_uppers = [1.5 * upper - 0.5 * step[0] for upper, step in zip(cur_uppers, steps)]
            new_lowers = [1.5 * lower - 0.5 * step[1] for lower, step in zip(cur_lowers, steps)]
            return tuple(new_uppers), tuple(new_lowers)

        uppers, lowers = lax.fori_loop(1, NSI - 1, sweep, (tuple(next_uppers), tuple(lowers)))

        lower_halves = [split(lower) for lower in lowers]
        nears = [times([lo], diag_rhs(*split(upper)))[0] for lo, upper in zip(lower_halves, uppers)]
        steps = [times([lo], diag_rhs(*split(near)))[0] for lo, near in zip(lower_halves, nears)]
        mixings = []
        for pair in range(NR // 2):
            lower = 1.5 * lowers[pair] - 0.5 * steps[pair]
            inv_root = lower / jnp.sqrt(scales[pair])
            half = halves_sum_exact(inv_root * drive_rows[pair])
            shift = jnp.sum(half * inv_root, axis=0, keepdims=True)
            transform = (K - 1.0) ** 0.5 * inv_root + shift
            mean = halves_sum_exact(transform) * (1.0 / K)
            mixings.append((1.0 / K + transform - mean).astype(bf16))
        mix_ref[0] = jnp.concatenate(mixings[:2], axis=1)
        mix_ref[1] = jnp.concatenate(mixings[2:], axis=1)

    def move(a):
        mix_lo = mix_ref[0]
        mix_hi = mix_ref[1]

        first_col = a * BLK
        for group in range(K // 16):
            members = pl.ds(group * 16, 16)
            cells = jnp.concatenate(
                [
                    tile_ref[members, lev, pl.ds(first_col, BLK), :].reshape(256, ROWS)
                    for lev in range(LEV)
                ],
                axis=1,
            )
            z_ref[:, members, :] = dot(swap, cells).astype(bf16).reshape(16, 16, 2 * ROWS)

        def mix_column(c, _):
            cells = z_ref[c]
            low = jnp.concatenate([cells * m for m in group_masks[:4]], axis=0)
            high = jnp.concatenate([cells * m for m in group_masks[4:]], axis=0)
            o_ref[c] = (dot(mix_lo, low) + dot(mix_hi, high)).astype(bf16)
            return 0

        lax.fori_loop(0, BLK, mix_column, 0, unroll=4)

        for group in range(K // 16):
            members = pl.ds(group * 16, 16)
            cells = dot(swap, o_ref[:, members, :].reshape(256, 2 * ROWS)).astype(bf16)
            for lev in range(LEV):
                mixed_ref[members, lev, pl.ds(first_col, BLK), :] = cells[
                    :, lev * ROWS : (lev + 1) * ROWS
                ].reshape(16, BLK, ROWS)

        each_peer(lambda target, _source: exit_copy(a, target, me).start())
        own_exit(a).start()

    def exit_copy(a, target, owner):
        return pltpu.make_async_remote_copy(
            src_ref=mixed_ref.at[target, :, pl.ds(a * BLK, BLK), :],
            dst_ref=out_ref.at[
                0, :, pl.ds(pl.multiple_of(owner * COLS + a * BLK, BLK), BLK), :
            ],
            send_sem=out_send.at[a, target],
            recv_sem=out_recv.at[a, owner],
            device_id=(target, gy),
            device_id_type=MESH,
        )

    def own_exit(a):
        return pltpu.make_async_copy(
            mixed_ref.at[me, :, pl.ds(a * BLK, BLK), :],
            out_ref.at[0, :, pl.ds(pl.multiple_of(me * COLS + a * BLK, BLK), BLK), :],
            own_sem.at[1 + a],
        )

    for a in range(2):
        solve(a)
        if a == 0:
            each_peer(lambda target, source: entry_copy(target, source).wait())
        move(a)

    for a in range(2):
        own_exit(a).wait()

        each_peer(lambda target, source: exit_copy(a, target, source).wait())


def local(state, obs_index, obs_count, obs_value, obs_var, radius):
    dma = pltpu.SemaphoreType.DMA
    return pl.pallas_call(
        kernel,
        out_shape=jax.ShapeDtypeStruct(state.shape, bf16),
        in_specs=[pl.BlockSpec(memory_space=pltpu.VMEM)] * 6,
        out_specs=pl.BlockSpec(memory_space=pl.ANY),
        scratch_shapes=[
            pltpu.VMEM((N_MEM, 1, OBS), jnp.int32),
            pltpu.VMEM((N_MEM, 1, OBS), f32),
            pltpu.VMEM((N_MEM, 1, OBS), f32),
            pltpu.VMEM((K, LEV, COLS, ROWS), bf16),
            pltpu.VMEM((K, LEV, COLS, ROWS), bf16),
            pltpu.VMEM((9, K, OBS), bf16),
            pltpu.VMEM((9, 8, OBS), f32),
            pltpu.VMEM((BLK, K, LEV * ROWS), bf16),
            pltpu.VMEM((BLK, K, LEV * ROWS), bf16),
            pltpu.VMEM((2, GRAM_ROWS, 2 * K), f32),
            pltpu.VMEM((2, K, 4 * K), bf16),
            dma((3,)),
            dma((N_MEM,)),
            dma((N_MEM,)),
            dma((N_MEM,)),
            dma((N_MEM,)),
            dma((N_MEM,)),
            dma((N_MEM,)),
            dma((8,)),
            dma((8,)),
            dma((8,)),
            dma((8,)),
            dma((2, N_MEM)),
            dma((2, N_MEM)),
        ],
        compiler_params=pltpu.CompilerParams(
            collective_id=0, has_side_effects=True, vmem_limit_bytes=24 * 2**20
        ),
    )(state, obs_index, obs_count, obs_value, obs_var, radius)


def solution(mesh):
    in_specs = (
        P("mem", None, None, "gy"),
        P("mem", "gy", None),
        P("mem", "gy"),
        P("mem", "gy", None),
        P("mem", "gy", None),
        P("mem", "gy"),
    )
    out_specs = P("mem", None, None, "gy")
    return jax.shard_map(local, mesh=mesh, in_specs=in_specs, out_specs=out_specs, check_vma=False)
```

```python
import functools

import jax
import jax.numpy as jnp
from jax import lax
from jax.experimental import pallas as pl
from jax.experimental.pallas import tpu as pltpu
from jax.sharding import PartitionSpec as P

K = 64
LEV = 2
ROWS = 128
COLS = 32
BLK = 16
OBS = 256
NSI = 10
N_MEM = 64
N_GY = 8
NR = ROWS // BLK
OWN = 4
BULK = (3, 5, 8)
VMEM_GRANT = 67043328 - 2300 * 1024
GRAM_ROWS = NR * K + 16

MESH = pl.DeviceIdType.MESH
f32 = jnp.float32
bf16 = jnp.bfloat16

SIDES = [(dx, dy) for dx in (-1, 0, 1) for dy in (-1, 0, 1) if (dx, dy) != (0, 0)]


def split(x):
    hi = x.astype(bf16)
    lo = (x - hi.astype(f32)).astype(bf16)
    return hi, lo


def dot(a, b):
    return jnp.dot(a, b, preferred_element_type=f32)


def dot_nt(a, b):
    return lax.dot_general(a, b, (((1,), (1,)), ((), ())), preferred_element_type=f32)


def rem(a, b):
    return lax.rem(a, jnp.int32(b))


def peers_of(me):
    z, x, c = lax.div(me, jnp.int32(8)), rem(lax.div(me, jnp.int32(2)), 4), rem(me, 2)
    planes = [rem(z + d, 8) * 8 for d in range(8)]
    order = [0, 1, 7, 2, 6, 3, 5, 4]

    def each(fn, first=0, last=8):
        if first == 0:
            for dz in order[1:]:
                fn(planes[dz] + x * 2 + c, planes[8 - dz] + x * 2 + c)

        def row(r, _):
            dx, dc = lax.div(r, jnp.int32(2)), rem(r, 2)
            there = rem(x + dx, 4) * 2 + rem(c + dc, 2)
            back = rem(x + 4 - dx, 4) * 2 + rem(c + 2 - dc, 2)
            for dz in order:
                fn(planes[dz] + there, planes[(8 - dz) % 8] + back)
            return 0

        lax.fori_loop(max(first, 1), last, row, 0)

    return each


def kernel(
    state_hbm, index_hbm, count_ref, value_hbm, var_hbm, radius_ref, out_ref,
    state_ref, index_ref, value_ref, var_ref,
    index_all, seen_ref, raw_ref,
    tile_ref, mixed_ref, ens_ref, halo_ref, z_ref, o_ref, gram_ref, mix_ref,
    arg_sem, own_sem, index_send, index_recv, seen_send, seen_recv, in_send, in_recv, meta_send, meta_recv, ens_send, ens_recv, out_send, out_recv,
):
    me = lax.axis_index("mem")
    gy = lax.axis_index("gy")
    barrier = pltpu.get_barrier_semaphore()

    arguments = [
        pltpu.make_async_copy(src, dst, arg_sem.at[i])
        for i, (src, dst) in enumerate(
            (
                (index_hbm, index_ref),
                (value_hbm, value_ref),
                (var_hbm, var_ref),
                (state_hbm, state_ref),
            )
        )
    ]
    for copy in arguments:
        copy.start()

    each_peer = peers_of(me)

    def greet(target, _source):
        pl.semaphore_signal(barrier, inc=1, device_id=(target, gy), device_id_type=MESH)

    each_peer(greet)
    for dx, dy in SIDES:
        if dy != 0:
            device = (rem(me + dx + N_MEM, N_MEM), rem(gy + dy + N_GY, N_GY))
            pl.semaphore_signal(barrier, inc=1, device_id=device, device_id_type=MESH)

    for copy in arguments:
        copy.wait()
    slots = index_ref[0]
    live = lax.broadcasted_iota(jnp.int32, (1, OBS), 1) < count_ref[0, 0]
    cell = lax.div(slots, jnp.int32(ROWS))
    meta = jnp.concatenate(
        [
            jnp.where(live, 1.0 / var_ref[0], 0.0),
            value_ref[0],
            rem(cell, COLS).astype(f32),
            rem(slots, ROWS).astype(f32),
            cell.astype(f32),
            jnp.zeros((3, OBS), f32),
        ],
        axis=0,
    )
    halo_ref[OWN] = meta
    radius = jnp.full((1, OBS), radius_ref[0, 0], jnp.int32).astype(f32)
    reach_sq = radius * radius
    pl.semaphore_wait(barrier, N_MEM - 1 + 6)

    def entry_copy(target, slot):
        return pltpu.make_async_remote_copy(
            src_ref=state_ref.at[0, :, pl.ds(pl.multiple_of(target * COLS, COLS), COLS), :],
            dst_ref=tile_ref.at[slot],
            send_sem=in_send.at[0],
            recv_sem=in_recv.at[0],
            device_id=(target, gy),
            device_id_type=MESH,
        )

    def side_copy(src, dst, send, recv, index):
        dx, dy = SIDES[index]
        slot = (dx + 1) * 3 + dy + 1
        device = (rem(me - dx + N_MEM, N_MEM), rem(gy - dy + N_GY, N_GY))
        return pltpu.make_async_remote_copy(
            src_ref=src,
            dst_ref=dst.at[slot],
            send_sem=send.at[index],
            recv_sem=recv.at[index],
            device_id=device,
            device_id_type=MESH,
        )

    def index_copy(target, slot):
        return pltpu.make_async_remote_copy(
            src_ref=index_ref.at[0],
            dst_ref=index_all.at[slot],
            send_sem=index_send.at[0],
            recv_sem=index_recv.at[0],
            device_id=(target, gy),
            device_id_type=MESH,
        )

    def seen_copy(target, slot):
        return pltpu.make_async_remote_copy(
            src_ref=seen_ref.at[target],
            dst_ref=raw_ref.at[slot],
            send_sem=seen_send.at[0],
            recv_sem=seen_recv.at[0],
            device_id=(target, gy),
            device_id_type=MESH,
        )

    def start_entry(target, _source):
        entry_copy(target, me).start()

    def finish_all(ref, send, recv):
        pltpu.make_async_remote_copy(
            src_ref=ref,
            dst_ref=ref,
            send_sem=send,
            recv_sem=recv,
            device_id=(rem(me + 1, N_MEM), gy),
            device_id_type=MESH,
        ).wait()

    each_peer(lambda target, _source: index_copy(target, me).start())
    meta_copies = [side_copy(halo_ref.at[OWN], halo_ref, meta_send, meta_recv, i) for i in range(8)]
    for copy in meta_copies:
        copy.start()
    each_peer(start_entry, 0, BULK[0])
    own_in = pltpu.make_async_copy(
        state_ref.at[0, :, pl.ds(pl.multiple_of(me * COLS, COLS), COLS), :],
        tile_ref.at[me],
        own_sem.at[0],
    )
    own_in.start()
    own_in.wait()
    index_all[me] = index_ref[0]
    finish_all(index_all.at[pl.ds(0, N_MEM - 1)], index_send.at[0], index_recv.at[0])

    row_iota = lax.broadcasted_iota(jnp.int32, (ROWS, OBS), 0)
    cell_iota = lax.broadcasted_iota(jnp.int32, (LEV * COLS, OBS), 0)

    def observe(tile, _):
        wanted = index_all[tile]
        pick_row = jnp.where(row_iota == (wanted & (ROWS - 1)), 1.0, 0.0).astype(bf16)
        cells = state_ref[0, :, pl.ds(pl.multiple_of(tile * COLS, COLS), COLS), :]
        rows = dot(cells.reshape(LEV * COLS, ROWS), pick_row)
        picked = jnp.where(cell_iota == (wanted >> 7), rows, 0.0)
        seen_ref[tile] = jnp.sum(picked, axis=0, keepdims=True)
        return 0

    lax.fori_loop(0, N_MEM, observe, 0, unroll=8)
    raw_ref[me] = seen_ref[me]
    each_peer(lambda target, _source: seen_copy(target, me).start())
    each_peer(start_entry, *BULK[:2])
    finish_all(raw_ref.at[pl.ds(0, N_MEM - 1)], seen_send.at[0], seen_recv.at[0])

    ens_ref[OWN] = raw_ref[:, 0, :].astype(bf16)
    ens_copies = [side_copy(ens_ref.at[OWN], ens_ref, ens_send, ens_recv, i) for i in range(8)]
    for copy in ens_copies:
        copy.start()
    each_peer(start_entry, *BULK[1:])

    left = lax.broadcasted_iota(jnp.int32, (K, 2 * K), 1) < K
    left_row = lax.broadcasted_iota(jnp.int32, (1, 2 * K), 1) < K
    lane = lax.broadcasted_iota(jnp.int32, (K, 2 * K), 1)
    eye = (lane % K == lax.broadcasted_iota(jnp.int32, (K, 2 * K), 0)).astype(f32)
    left_bf = jnp.where(left, 1.0, 0.0).astype(bf16)
    right_bf = jnp.where(left, 0.0, 1.0).astype(bf16)
    i_row = lax.broadcasted_iota(jnp.int32, (256, 256), 0)
    i_col = lax.broadcasted_iota(jnp.int32, (256, 256), 1)
    swap = jnp.where(
        (i_row // 16 == i_col % 16) & (i_row % 16 == i_col // 16), 1.0, 0.0
    ).astype(bf16)
    centre_r = lax.broadcasted_iota(jnp.int32, (NR, OBS), 0).astype(f32) * BLK + (BLK - 1) / 2.0
    row_group = lax.broadcasted_iota(jnp.int32, (K, 2 * ROWS), 1) % ROWS // BLK
    group_masks = [jnp.where(row_group == r, 1.0, 0.0).astype(bf16) for r in range(NR)]

    def halves_sum(x):
        total = jnp.sum(x, axis=1, keepdims=True)
        first = jnp.sum(jnp.where(left, x, 0.0), axis=1, keepdims=True)
        return jnp.where(left, first, total - first)

    def halves_sum_exact(x):
        first = jnp.sum(jnp.where(left, x, 0.0), axis=1, keepdims=True)
        second = jnp.sum(jnp.where(left, 0.0, x), axis=1, keepdims=True)
        return jnp.where(left, first, second)

    def weighted(slot, dx, dy, a):
        ens = ens_ref[slot].astype(f32)
        about = halo_ref[slot]
        centre = jnp.sum(ens, axis=0, keepdims=True) * (1.0 / K)
        spread = ens - centre
        innovation = about[1:2] - centre
        inside = (me + dx >= 0) & (me + dx < N_MEM) & (gy + dy >= 0) & (gy + dy < N_GY)
        weight = about[0:1] * jnp.where(inside, 1.0, 0.0)
        centre_c = a * BLK + (BLK - 1) / 2.0
        gap_c = (dx * COLS) * 1.0 + about[2:3] - centre_c
        gap_r = (dy * ROWS) * 1.0 + about[3:4] - centre_r
        taper = jnp.square(jnp.maximum(1.0 - (gap_c * gap_c + gap_r * gap_r) / reach_sq, 0.0))
        rho = taper * weight
        drive = jnp.concatenate([rho * innovation, jnp.zeros((8, OBS), f32)], axis=0)
        hi, lo = split(spread)
        return rho, spread, drive, jnp.concatenate([hi, lo], axis=0)

    def product(parts, both):
        hi, lo = split(jnp.concatenate(parts, axis=0))
        return dot_nt(hi, both) + dot_nt(lo, both)

    for a in range(2):
        rho, spread, drive, both = weighted(OWN, 0, 0, a)
        gram_ref[a] = product([rho[r : r + 1] * spread for r in range(NR)] + [drive], both)
    for copy in meta_copies:
        copy.wait()
    for copy in ens_copies:
        copy.wait()

    def folded(block):
        return block + pltpu.roll(block, K, 1)

    def diag_rhs(hi, lo):
        return jnp.concatenate(
            [
                jnp.concatenate([hi * left_bf, hi * right_bf], axis=0),
                jnp.concatenate([lo * left_bf, lo * right_bf], axis=0),
            ],
            axis=1,
        )

    def times(parts, rhs):
        out = dot(jnp.concatenate([x for part in parts for x in part], axis=0), rhs)
        sides = out[:, : 2 * K] + out[:, 2 * K :]
        return [sides[2 * i * K : (2 * i + 1) * K] + sides[(2 * i + 1) * K : 2 * (i + 1) * K] for i in range(len(parts))]

    def solve(a):
        uppers, lowers, scales, drive_rows = [], [], [], []
        dx = 2 * a - 1
        side = 6 * a + 1
        rho, spread, drive, both = weighted(side, dx, 0, a)
        gram_ref[a] += product([rho[r : r + 1] * spread for r in range(NR)] + [drive], both)
        for dy, r in ((-1, 0), (1, NR - 1)):
            for slot, step in ((OWN + dy, 0), (side + dy, dx)):
                rho, spread, drive, both = weighted(slot, step, dy, a)
                part = product([rho[r : r + 1] * spread, drive], both)
                gram_ref[a, r * K : (r + 1) * K, :] += part[:K]
                gram_ref[a, NR * K :, :] += part[K:]

        drives = folded(gram_ref[a, NR * K :, :])
        for pair in range(NR // 2):
            r = 2 * pair
            first = folded(gram_ref[a, r * K : (r + 1) * K, :])
            second = folded(gram_ref[a, (r + 1) * K : (r + 2) * K, :])
            system = (K - 1.0) * eye + jnp.where(left, first, second)
            diagonal = jnp.sum(system * eye, axis=0, keepdims=True)
            trace_l = jnp.sum(jnp.where(left_row, diagonal, 0.0), axis=1, keepdims=True)
            trace_r = jnp.sum(jnp.where(left_row, 0.0, diagonal), axis=1, keepdims=True)
            scale = jnp.where(left_row, trace_l, trace_r)
            scales.append(scale)
            drive_rows.append(jnp.where(left_row, drives[r : r + 1], drives[r + 1 : r + 2]))
            uppers.append(system / scale)

        next_uppers = []
        for upper in uppers:
            halves = split(upper)
            next_uppers.append(1.5 * upper - 0.5 * times([halves], diag_rhs(*halves))[0])
            lowers.append(1.5 * eye - 0.5 * upper)

        def sweep(_, carry):
            cur_uppers, cur_lowers = carry
            upper_halves = [split(upper) for upper in cur_uppers]
            lower_halves = [split(lower) for lower in cur_lowers]
            nears = [times([lo], diag_rhs(*up))[0] for lo, up in zip(lower_halves, upper_halves)]
            steps = [
                times([up, lo], diag_rhs(*split(near)))
                for up, lo, near in zip(upper_halves, lower_halves, nears)
            ]
            new_uppers = [1.5 * upper - 0.5 * step[0] for upper, step in zip(cur_uppers, steps)]
            new_lowers = [1.5 * lower - 0.5 * step[1] for lower, step in zip(cur_lowers, steps)]
            return tuple(new_uppers), tuple(new_lowers)

        uppers, lowers = lax.fori_loop(1, NSI - 1, sweep, (tuple(next_uppers), tuple(lowers)))

        lower_halves = [split(lower) for lower in lowers]
        nears = [times([lo], diag_rhs(*split(upper)))[0] for lo, upper in zip(lower_halves, uppers)]
        steps = [times([lo], diag_rhs(*split(near)))[0] for lo, near in zip(lower_halves, nears)]
        mixings = []
        for pair in range(NR // 2):
            lower = 1.5 * lowers[pair] - 0.5 * steps[pair]
            inv_root = lower / jnp.sqrt(scales[pair])
            half = halves_sum_exact(inv_root * drive_rows[pair])
            shift = jnp.sum(half * inv_root, axis=0, keepdims=True)
            transform = (K - 1.0) ** 0.5 * inv_root + shift
            mean = halves_sum_exact(transform) * (1.0 / K)
            mixings.append((1.0 / K + transform - mean).astype(bf16))
        mix_ref[0] = jnp.concatenate(mixings[:2], axis=1)
        mix_ref[1] = jnp.concatenate(mixings[2:], axis=1)

    def move(a):
        mix_lo = mix_ref[0]
        mix_hi = mix_ref[1]

        first_col = a * BLK
        for group in range(K // 16):
            members = pl.ds(group * 16, 16)
            cells = jnp.concatenate(
                [
                    tile_ref[members, lev, pl.ds(first_col, BLK), :].reshape(256, ROWS)
                    for lev in range(LEV)
                ],
                axis=1,
            )
            z_ref[:, members, :] = dot(swap, cells).astype(bf16).reshape(16, 16, 2 * ROWS)

        def mix_column(c, _):
            cells = z_ref[c]
            low = jnp.concatenate([cells * m for m in group_masks[:4]], axis=0)
            high = jnp.concatenate([cells * m for m in group_masks[4:]], axis=0)
            o_ref[c] = (dot(mix_lo, low) + dot(mix_hi, high)).astype(bf16)
            return 0

        lax.fori_loop(0, BLK, mix_column, 0, unroll=4)

        for group in range(K // 16):
            members = pl.ds(group * 16, 16)
            cells = dot(swap, o_ref[:, members, :].reshape(256, 2 * ROWS)).astype(bf16)
            for lev in range(LEV):
                mixed_ref[members, lev, pl.ds(first_col, BLK), :] = cells[
                    :, lev * ROWS : (lev + 1) * ROWS
                ].reshape(16, BLK, ROWS)

        each_peer(lambda target, _source: exit_copy(a, target, me).start())
        own_exit(a).start()

    def exit_copy(a, target, owner):
        return pltpu.make_async_remote_copy(
            src_ref=mixed_ref.at[target, :, pl.ds(a * BLK, BLK), :],
            dst_ref=out_ref.at[
                0, :, pl.ds(pl.multiple_of(owner * COLS + a * BLK, BLK), BLK), :
            ],
            send_sem=out_send.at[a],
            recv_sem=out_recv.at[a],
            device_id=(target, gy),
            device_id_type=MESH,
        )

    def own_exit(a):
        return pltpu.make_async_copy(
            mixed_ref.at[me, :, pl.ds(a * BLK, BLK), :],
            out_ref.at[0, :, pl.ds(pl.multiple_of(me * COLS + a * BLK, BLK), BLK), :],
            own_sem.at[1 + a],
        )

    for a in range(2):
        solve(a)
        if a == 0:
            finish_all(tile_ref.at[pl.ds(0, N_MEM - 1)], in_send.at[0], in_recv.at[0])
        move(a)

    for a in range(2):
        own_exit(a).wait()

        band_cells = mixed_ref.at[pl.ds(0, N_MEM - 1), :, pl.ds(a * BLK, BLK), :]
        finish_all(band_cells, out_send.at[a], out_recv.at[a])


def local(state, obs_index, obs_count, obs_value, obs_var, radius):
    dma = pltpu.SemaphoreType.DMA
    return pl.pallas_call(
        kernel,
        out_shape=pltpu.VMEM(state.shape, bf16),
        in_specs=[
            pl.BlockSpec(memory_space=pl.ANY),
            pl.BlockSpec(memory_space=pl.ANY),
            pl.BlockSpec(memory_space=pltpu.SMEM),
            pl.BlockSpec(memory_space=pl.ANY),
            pl.BlockSpec(memory_space=pl.ANY),
            pl.BlockSpec(memory_space=pltpu.SMEM),
        ],
        out_specs=pl.BlockSpec(memory_space=pl.ANY),
        scratch_shapes=[
            pltpu.VMEM(state.shape, bf16),
            pltpu.VMEM((1, 1, OBS), jnp.int32),
            pltpu.VMEM((1, 1, OBS), f32),
            pltpu.VMEM((1, 1, OBS), f32),
            pltpu.VMEM((N_MEM, 1, OBS), jnp.int32),
            pltpu.VMEM((N_MEM, 1, OBS), f32),
            pltpu.VMEM((N_MEM, 1, OBS), f32),
            pltpu.VMEM((K, LEV, COLS, ROWS), bf16),
            pltpu.VMEM((K, LEV, COLS, ROWS), bf16),
            pltpu.VMEM((9, K, OBS), bf16),
            pltpu.VMEM((9, 8, OBS), f32),
            pltpu.VMEM((BLK, K, LEV * ROWS), bf16),
            pltpu.VMEM((BLK, K, LEV * ROWS), bf16),
            pltpu.VMEM((2, GRAM_ROWS, 2 * K), f32),
            pltpu.VMEM((2, K, 4 * K), bf16),
            dma((4,)),
            dma((3,)),
            dma((1,)),
            dma((1,)),
            dma((1,)),
            dma((1,)),
            dma((1,)),
            dma((1,)),
            dma((8,)),
            dma((8,)),
            dma((8,)),
            dma((8,)),
            dma((2,)),
            dma((2,)),
        ],
        compiler_params=pltpu.CompilerParams(
            collective_id=0, has_side_effects=True, vmem_limit_bytes=VMEM_GRANT
        ),
    )(state, obs_index, obs_count, obs_value, obs_var, radius)


def solution(mesh):
    in_specs = (
        P("mem", None, None, "gy"),
        P("mem", "gy", None),
        P("mem", "gy"),
        P("mem", "gy", None),
        P("mem", "gy", None),
        P("mem", "gy"),
    )
    out_specs = P("mem", None, None, "gy")
    return jax.shard_map(local, mesh=mesh, in_specs=in_specs, out_specs=out_specs, check_vma=False)
```

```python
import functools

import jax
import jax.numpy as jnp
from jax import lax
from jax.experimental import pallas as pl
from jax.experimental.pallas import tpu as pltpu
from jax.sharding import PartitionSpec as P

K = 64
LEV = 2
ROWS = 128
COLS = 32
BLK = 16
OBS = 256
NSI = 10
N_MEM = 64
N_GY = 8
NR = ROWS // BLK
OWN = 4
BULK = (4, 6, 8)
VMEM_GRANT = 67043328 - 2300 * 1024
GRAM_ROWS = NR * K + 16

MESH = pl.DeviceIdType.MESH
f32 = jnp.float32
bf16 = jnp.bfloat16

SIDES = [(dx, dy) for dx in (-1, 0, 1) for dy in (-1, 0, 1) if (dx, dy) != (0, 0)]


def split(x):
    hi = x.astype(bf16)
    lo = (x - hi.astype(f32)).astype(bf16)
    return hi, lo


def dot(a, b):
    return jnp.dot(a, b, preferred_element_type=f32)


def dot_nt(a, b):
    return lax.dot_general(a, b, (((1,), (1,)), ((), ())), preferred_element_type=f32)


def rem(a, b):
    return lax.rem(a, jnp.int32(b))


def peers_of(me):
    z, x, c = lax.div(me, jnp.int32(8)), rem(lax.div(me, jnp.int32(2)), 4), rem(me, 2)
    planes = [rem(z + d, 8) * 8 for d in range(8)]
    order = [0, 1, 7, 2, 6, 3, 5, 4]

    def each(fn, first=0, last=8):
        if first == 0:
            for dz in order[1:]:
                fn(planes[dz] + x * 2 + c, planes[8 - dz] + x * 2 + c)

        def row(r, _):
            dx, dc = lax.div(r, jnp.int32(2)), rem(r, 2)
            there = rem(x + dx, 4) * 2 + rem(c + dc, 2)
            back = rem(x + 4 - dx, 4) * 2 + rem(c + 2 - dc, 2)
            for dz in order:
                fn(planes[dz] + there, planes[(8 - dz) % 8] + back)
            return 0

        lax.fori_loop(max(first, 1), last, row, 0)

    return each


def kernel(
    state_hbm, index_hbm, count_ref, value_hbm, var_hbm, radius_ref, out_ref,
    state_ref, index_ref, value_ref, var_ref,
    index_all, seen_ref, raw_ref,
    tile_ref, mixed_ref, ens_ref, halo_ref, z_ref, o_ref, gram_ref, mix_ref,
    arg_sem, own_sem, index_send, index_recv, seen_send, seen_recv, in_send, in_recv, meta_send, meta_recv, ens_send, ens_recv, out_send, out_recv,
):
    me = lax.axis_index("mem")
    gy = lax.axis_index("gy")
    barrier = pltpu.get_barrier_semaphore()

    arguments = [
        pltpu.make_async_copy(src, dst, arg_sem.at[i])
        for i, (src, dst) in enumerate(
            (
                (index_hbm, index_ref),
                (value_hbm, value_ref),
                (var_hbm, var_ref),
                (state_hbm, state_ref),
            )
        )
    ]
    for copy in arguments:
        copy.start()

    each_peer = peers_of(me)

    def greet(target, _source):
        pl.semaphore_signal(barrier, inc=1, device_id=(target, gy), device_id_type=MESH)

    each_peer(greet)
    for dx, dy in SIDES:
        if dy != 0:
            device = (rem(me + dx + N_MEM, N_MEM), rem(gy + dy + N_GY, N_GY))
            pl.semaphore_signal(barrier, inc=1, device_id=device, device_id_type=MESH)

    for copy in arguments:
        copy.wait()
    slots = index_ref[0]
    live = lax.broadcasted_iota(jnp.int32, (1, OBS), 1) < count_ref[0, 0]
    cell = lax.div(slots, jnp.int32(ROWS))
    meta = jnp.concatenate(
        [
            jnp.where(live, 1.0 / var_ref[0], 0.0),
            value_ref[0],
            rem(cell, COLS).astype(f32),
            rem(slots, ROWS).astype(f32),
            cell.astype(f32),
            jnp.zeros((3, OBS), f32),
        ],
        axis=0,
    )
    halo_ref[OWN] = meta
    radius = jnp.full((1, OBS), radius_ref[0, 0], jnp.int32).astype(f32)
    reach_sq = radius * radius
    pl.semaphore_wait(barrier, N_MEM - 1 + 6)

    def entry_copy(target, slot):
        return pltpu.make_async_remote_copy(
            src_ref=state_ref.at[0, :, pl.ds(pl.multiple_of(target * COLS, COLS), COLS), :],
            dst_ref=tile_ref.at[slot],
            send_sem=in_send.at[0],
            recv_sem=in_recv.at[0],
            device_id=(target, gy),
            device_id_type=MESH,
        )

    def side_copy(src, dst, send, recv, index):
        dx, dy = SIDES[index]
        slot = (dx + 1) * 3 + dy + 1
        device = (rem(me - dx + N_MEM, N_MEM), rem(gy - dy + N_GY, N_GY))
        return pltpu.make_async_remote_copy(
            src_ref=src,
            dst_ref=dst.at[slot],
            send_sem=send.at[index],
            recv_sem=recv.at[index],
            device_id=device,
            device_id_type=MESH,
        )

    def index_copy(target, slot):
        return pltpu.make_async_remote_copy(
            src_ref=index_ref.at[0],
            dst_ref=index_all.at[slot],
            send_sem=index_send.at[0],
            recv_sem=index_recv.at[0],
            device_id=(target, gy),
            device_id_type=MESH,
        )

    def seen_copy(target, slot):
        return pltpu.make_async_remote_copy(
            src_ref=seen_ref.at[target],
            dst_ref=raw_ref.at[slot],
            send_sem=seen_send.at[0],
            recv_sem=seen_recv.at[0],
            device_id=(target, gy),
            device_id_type=MESH,
        )

    def start_entry(target, _source):
        entry_copy(target, me).start()

    def finish_all(ref, send, recv):
        pltpu.make_async_remote_copy(
            src_ref=ref,
            dst_ref=ref,
            send_sem=send,
            recv_sem=recv,
            device_id=(rem(me + 1, N_MEM), gy),
            device_id_type=MESH,
        ).wait()

    each_peer(lambda target, _source: index_copy(target, me).start())
    meta_copies = [side_copy(halo_ref.at[OWN], halo_ref, meta_send, meta_recv, i) for i in range(8)]
    for copy in meta_copies:
        copy.start()
    each_peer(start_entry, 0, BULK[0])
    own_in = pltpu.make_async_copy(
        state_ref.at[0, :, pl.ds(pl.multiple_of(me * COLS, COLS), COLS), :],
        tile_ref.at[me],
        own_sem.at[0],
    )
    own_in.start()
    own_in.wait()
    index_all[me] = index_ref[0]
    finish_all(index_all.at[pl.ds(0, N_MEM - 1)], index_send.at[0], index_recv.at[0])

    row_iota = lax.broadcasted_iota(jnp.int32, (ROWS, OBS), 0)
    cell_iota = lax.broadcasted_iota(jnp.int32, (LEV * COLS, OBS), 0)

    def observe(tile, _):
        wanted = index_all[tile]
        pick_row = jnp.where(row_iota == (wanted & (ROWS - 1)), 1.0, 0.0).astype(bf16)
        cells = state_ref[0, :, pl.ds(pl.multiple_of(tile * COLS, COLS), COLS), :]
        rows = dot(cells.reshape(LEV * COLS, ROWS), pick_row)
        picked = jnp.where(cell_iota == (wanted >> 7), rows, 0.0)
        seen_ref[tile] = jnp.sum(picked, axis=0, keepdims=True)
        return 0

    lax.fori_loop(0, N_MEM, observe, 0, unroll=8)
    raw_ref[me] = seen_ref[me]
    each_peer(lambda target, _source: seen_copy(target, me).start())
    each_peer(start_entry, *BULK[:2])
    finish_all(raw_ref.at[pl.ds(0, N_MEM - 1)], seen_send.at[0], seen_recv.at[0])

    ens_ref[OWN] = raw_ref[:, 0, :].astype(bf16)
    ens_copies = [side_copy(ens_ref.at[OWN], ens_ref, ens_send, ens_recv, i) for i in range(8)]
    for copy in ens_copies:
        copy.start()
    each_peer(start_entry, *BULK[1:])

    left = lax.broadcasted_iota(jnp.int32, (K, 2 * K), 1) < K
    left_row = lax.broadcasted_iota(jnp.int32, (1, 2 * K), 1) < K
    lane = lax.broadcasted_iota(jnp.int32, (K, 2 * K), 1)
    eye = (lane % K == lax.broadcasted_iota(jnp.int32, (K, 2 * K), 0)).astype(f32)
    left_bf = jnp.where(left, 1.0, 0.0).astype(bf16)
    right_bf = jnp.where(left, 0.0, 1.0).astype(bf16)
    i_row = lax.broadcasted_iota(jnp.int32, (256, 256), 0)
    i_col = lax.broadcasted_iota(jnp.int32, (256, 256), 1)
    swap = jnp.where(
        (i_row // 16 == i_col % 16) & (i_row % 16 == i_col // 16), 1.0, 0.0
    ).astype(bf16)
    centre_r = lax.broadcasted_iota(jnp.int32, (NR, OBS), 0).astype(f32) * BLK + (BLK - 1) / 2.0
    row_group = lax.broadcasted_iota(jnp.int32, (K, 2 * ROWS), 1) % ROWS // BLK
    group_masks = [jnp.where(row_group == r, 1.0, 0.0).astype(bf16) for r in range(NR)]

    def halves_sum(x):
        total = jnp.sum(x, axis=1, keepdims=True)
        first = jnp.sum(jnp.where(left, x, 0.0), axis=1, keepdims=True)
        return jnp.where(left, first, total - first)

    def halves_sum_exact(x):
        first = jnp.sum(jnp.where(left, x, 0.0), axis=1, keepdims=True)
        second = jnp.sum(jnp.where(left, 0.0, x), axis=1, keepdims=True)
        return jnp.where(left, first, second)

    def weighted(slot, dx, dy, a):
        ens = ens_ref[slot].astype(f32)
        about = halo_ref[slot]
        centre = jnp.sum(ens, axis=0, keepdims=True) * (1.0 / K)
        spread = ens - centre
        innovation = about[1:2] - centre
        inside = (me + dx >= 0) & (me + dx < N_MEM) & (gy + dy >= 0) & (gy + dy < N_GY)
        weight = about[0:1] * jnp.where(inside, 1.0, 0.0)
        centre_c = a * BLK + (BLK - 1) / 2.0
        gap_c = (dx * COLS) * 1.0 + about[2:3] - centre_c
        gap_r = (dy * ROWS) * 1.0 + about[3:4] - centre_r
        taper = jnp.square(jnp.maximum(1.0 - (gap_c * gap_c + gap_r * gap_r) / reach_sq, 0.0))
        rho = taper * weight
        drive = jnp.concatenate([rho * innovation, jnp.zeros((8, OBS), f32)], axis=0)
        hi, lo = split(spread)
        return rho, spread, drive, jnp.concatenate([hi, lo], axis=0)

    def product(parts, both):
        hi, lo = split(jnp.concatenate(parts, axis=0))
        return dot_nt(hi, both) + dot_nt(lo, both)

    for a in range(2):
        rho, spread, drive, both = weighted(OWN, 0, 0, a)
        gram_ref[a] = product([rho[r : r + 1] * spread for r in range(NR)] + [drive], both)
    for copy in meta_copies:
        copy.wait()
    for copy in ens_copies:
        copy.wait()

    def folded(block):
        return block + pltpu.roll(block, K, 1)

    def diag_rhs(hi, lo):
        return jnp.concatenate(
            [
                jnp.concatenate([hi * left_bf, hi * right_bf], axis=0),
                jnp.concatenate([lo * left_bf, lo * right_bf], axis=0),
            ],
            axis=1,
        )

    def times(parts, rhs):
        out = dot(jnp.concatenate([x for part in parts for x in part], axis=0), rhs)
        sides = out[:, : 2 * K] + out[:, 2 * K :]
        return [sides[2 * i * K : (2 * i + 1) * K] + sides[(2 * i + 1) * K : 2 * (i + 1) * K] for i in range(len(parts))]

    def solve(a):
        uppers, lowers, scales, drive_rows = [], [], [], []
        dx = 2 * a - 1
        side = 6 * a + 1
        rho, spread, drive, both = weighted(side, dx, 0, a)
        gram_ref[a] += product([rho[r : r + 1] * spread for r in range(NR)] + [drive], both)
        for dy, r in ((-1, 0), (1, NR - 1)):
            for slot, step in ((OWN + dy, 0), (side + dy, dx)):
                rho, spread, drive, both = weighted(slot, step, dy, a)
                part = product([rho[r : r + 1] * spread, drive], both)
                gram_ref[a, r * K : (r + 1) * K, :] += part[:K]
                gram_ref[a, NR * K :, :] += part[K:]

        drives = folded(gram_ref[a, NR * K :, :])
        for pair in range(NR // 2):
            r = 2 * pair
            first = folded(gram_ref[a, r * K : (r + 1) * K, :])
            second = folded(gram_ref[a, (r + 1) * K : (r + 2) * K, :])
            system = (K - 1.0) * eye + jnp.where(left, first, second)
            diagonal = jnp.sum(system * eye, axis=0, keepdims=True)
            trace_l = jnp.sum(jnp.where(left_row, diagonal, 0.0), axis=1, keepdims=True)
            trace_r = jnp.sum(jnp.where(left_row, 0.0, diagonal), axis=1, keepdims=True)
            scale = jnp.where(left_row, trace_l, trace_r)
            scales.append(scale)
            drive_rows.append(jnp.where(left_row, drives[r : r + 1], drives[r + 1 : r + 2]))
            uppers.append(system / scale)

        next_uppers = []
        for upper in uppers:
            halves = split(upper)
            next_uppers.append(1.5 * upper - 0.5 * times([halves], diag_rhs(*halves))[0])
            lowers.append(1.5 * eye - 0.5 * upper)

        def sweep(_, carry):
            cur_uppers, cur_lowers = carry
            upper_halves = [split(upper) for upper in cur_uppers]
            lower_halves = [split(lower) for lower in cur_lowers]
            nears = [times([lo], diag_rhs(*up))[0] for lo, up in zip(lower_halves, upper_halves)]
            steps = [
                times([up, lo], diag_rhs(*split(near)))
                for up, lo, near in zip(upper_halves, lower_halves, nears)
            ]
            new_uppers = [1.5 * upper - 0.5 * step[0] for upper, step in zip(cur_uppers, steps)]
            new_lowers = [1.5 * lower - 0.5 * step[1] for lower, step in zip(cur_lowers, steps)]
            return tuple(new_uppers), tuple(new_lowers)

        uppers, lowers = lax.fori_loop(1, NSI - 1, sweep, (tuple(next_uppers), tuple(lowers)))

        lower_halves = [split(lower) for lower in lowers]
        nears = [times([lo], diag_rhs(*split(upper)))[0] for lo, upper in zip(lower_halves, uppers)]
        steps = [times([lo], diag_rhs(*split(near)))[0] for lo, near in zip(lower_halves, nears)]
        mixings = []
        for pair in range(NR // 2):
            lower = 1.5 * lowers[pair] - 0.5 * steps[pair]
            inv_root = lower / jnp.sqrt(scales[pair])
            half = halves_sum_exact(inv_root * drive_rows[pair])
            shift = jnp.sum(half * inv_root, axis=0, keepdims=True)
            transform = (K - 1.0) ** 0.5 * inv_root + shift
            mean = halves_sum_exact(transform) * (1.0 / K)
            mixings.append((1.0 / K + transform - mean).astype(bf16))
        mix_ref[0] = jnp.concatenate(mixings[:2], axis=1)
        mix_ref[1] = jnp.concatenate(mixings[2:], axis=1)

    def move(a):
        mix_lo = mix_ref[0]
        mix_hi = mix_ref[1]

        first_col = a * BLK
        for group in range(K // 16):
            members = pl.ds(group * 16, 16)
            cells = jnp.concatenate(
                [
                    tile_ref[members, lev, pl.ds(first_col, BLK), :].reshape(256, ROWS)
                    for lev in range(LEV)
                ],
                axis=1,
            )
            z_ref[:, members, :] = dot(swap, cells).astype(bf16).reshape(16, 16, 2 * ROWS)

        def mix_column(c, _):
            cells = z_ref[c]
            low = jnp.concatenate([cells * m for m in group_masks[:4]], axis=0)
            high = jnp.concatenate([cells * m for m in group_masks[4:]], axis=0)
            o_ref[c] = (dot(mix_lo, low) + dot(mix_hi, high)).astype(bf16)
            return 0

        lax.fori_loop(0, BLK, mix_column, 0, unroll=4)

        for group in range(K // 16):
            members = pl.ds(group * 16, 16)
            cells = dot(swap, o_ref[:, members, :].reshape(256, 2 * ROWS)).astype(bf16)
            for lev in range(LEV):
                mixed_ref[members, lev, pl.ds(first_col, BLK), :] = cells[
                    :, lev * ROWS : (lev + 1) * ROWS
                ].reshape(16, BLK, ROWS)

        each_peer(lambda target, _source: exit_copy(a, target, me).start())
        own_exit(a).start()

    def exit_copy(a, target, owner):
        return pltpu.make_async_remote_copy(
            src_ref=mixed_ref.at[target, :, pl.ds(a * BLK, BLK), :],
            dst_ref=out_ref.at[
                0, :, pl.ds(pl.multiple_of(owner * COLS + a * BLK, BLK), BLK), :
            ],
            send_sem=out_send.at[a],
            recv_sem=out_recv.at[a],
            device_id=(target, gy),
            device_id_type=MESH,
        )

    def own_exit(a):
        return pltpu.make_async_copy(
            mixed_ref.at[me, :, pl.ds(a * BLK, BLK), :],
            out_ref.at[0, :, pl.ds(pl.multiple_of(me * COLS + a * BLK, BLK), BLK), :],
            own_sem.at[1 + a],
        )

    for a in range(2):
        solve(a)
        if a == 0:
            finish_all(tile_ref.at[pl.ds(0, N_MEM - 1)], in_send.at[0], in_recv.at[0])
        move(a)

    for a in range(2):
        own_exit(a).wait()

        band_cells = mixed_ref.at[pl.ds(0, N_MEM - 1), :, pl.ds(a * BLK, BLK), :]
        finish_all(band_cells, out_send.at[a], out_recv.at[a])


def local(state, obs_index, obs_count, obs_value, obs_var, radius):
    dma = pltpu.SemaphoreType.DMA
    return pl.pallas_call(
        kernel,
        out_shape=pltpu.VMEM(state.shape, bf16),
        in_specs=[
            pl.BlockSpec(memory_space=pl.ANY),
            pl.BlockSpec(memory_space=pl.ANY),
            pl.BlockSpec(memory_space=pltpu.SMEM),
            pl.BlockSpec(memory_space=pl.ANY),
            pl.BlockSpec(memory_space=pl.ANY),
            pl.BlockSpec(memory_space=pltpu.SMEM),
        ],
        out_specs=pl.BlockSpec(memory_space=pl.ANY),
        scratch_shapes=[
            pltpu.VMEM(state.shape, bf16),
            pltpu.VMEM((1, 1, OBS), jnp.int32),
            pltpu.VMEM((1, 1, OBS), f32),
            pltpu.VMEM((1, 1, OBS), f32),
            pltpu.VMEM((N_MEM, 1, OBS), jnp.int32),
            pltpu.VMEM((N_MEM, 1, OBS), f32),
            pltpu.VMEM((N_MEM, 1, OBS), f32),
            pltpu.VMEM((K, LEV, COLS, ROWS), bf16),
            pltpu.VMEM((K, LEV, COLS, ROWS), bf16),
            pltpu.VMEM((9, K, OBS), bf16),
            pltpu.VMEM((9, 8, OBS), f32),
            pltpu.VMEM((BLK, K, LEV * ROWS), bf16),
            pltpu.VMEM((BLK, K, LEV * ROWS), bf16),
            pltpu.VMEM((2, GRAM_ROWS, 2 * K), f32),
            pltpu.VMEM((2, K, 4 * K), bf16),
            dma((4,)),
            dma((3,)),
            dma((1,)),
            dma((1,)),
            dma((1,)),
            dma((1,)),
            dma((1,)),
            dma((1,)),
            dma((8,)),
            dma((8,)),
            dma((8,)),
            dma((8,)),
            dma((2,)),
            dma((2,)),
        ],
        compiler_params=pltpu.CompilerParams(
            collective_id=0, has_side_effects=True, vmem_limit_bytes=VMEM_GRANT
        ),
    )(state, obs_index, obs_count, obs_value, obs_var, radius)


def solution(mesh):
    in_specs = (
        P("mem", None, None, "gy"),
        P("mem", "gy", None),
        P("mem", "gy"),
        P("mem", "gy", None),
        P("mem", "gy", None),
        P("mem", "gy"),
    )
    out_specs = P("mem", None, None, "gy")
    return jax.shard_map(local, mesh=mesh, in_specs=in_specs, out_specs=out_specs, check_vma=False)
```
